256 devices in a mesh: grp: 4 (over y_hi, core), blk: 64 (over z, y_lo, x).
Axes of the slice: x: 4, y: 4 (y_hi: 2, y_lo: 2; y = y_hi * 2 + y_lo), z: 8, core: 2. Of those that a mesh axis runs over, the one named last changes fastest.
Arguments:
- image_embed: bfloat16 [8192, 1152], P(('grp', 'blk')), may hold values from -0.53033009 to 0.53033009
- text_feature: bfloat16 [8192, 1152], P(('grp', 'blk')), may hold values from -0.18 to 0.18
- text_head: bfloat16 [1152, 1152], replicated, may hold values from -0.176776695 to 0.176776695
- log_scale: float32 [1], replicated, may hold values from 4 to 4.8
- bias: float32 [1], replicated, may hold values from -10 to -6
Outputs:
- grad_image: bfloat16 [8192, 1152], P(('grp', 'blk'))
- grad_text: bfloat16 [8192, 1152], P(('grp', 'blk'))
- grad_head: float32 [1152, 1152], P('blk')
The draws below stay inside these ranges and needn't reach their ends.
All inputs are finite; a program needn't handle non-finite values.
Results may differ from the reference program's by a relative error of at most 0.018.
Values may be sent and summed in bfloat16 or wider, within the bound.
A program may use at most 64 MiB of HBM per device.

```python
import math
import jax
import jax.numpy as jnp
from jax import lax

D = 1152
TOK_DEV = 32
B = 8192
N_GRP = 4
N_BLK = 64


def base_draw(key):
    head_key = jax.random.fold_in(key, 101)
    feature_key = jax.random.fold_in(key, 102)
    head_matrix = jax.random.normal(head_key, (D, D), jnp.float32) / math.sqrt(D)
    feature = jax.random.normal(feature_key, (B, D), jnp.float32) * 0.03
    head_bound = 6.0 / math.sqrt(D)
    return (jnp.clip(head_matrix, -head_bound, head_bound), jnp.clip(feature, -0.18, 0.18))


def draw_text_head(key, part):
    head_matrix, feature = base_draw(key)
    return head_matrix.astype(jnp.bfloat16)


def draw_text_feature(key, part):
    head_matrix, feature = base_draw(key)
    return feature.astype(jnp.bfloat16)


def draw_image_embed(key, part):
    head_matrix, feature = base_draw(key)
    projected = jnp.dot(feature, head_matrix, precision=lax.Precision.HIGHEST)
    direction = projected / jnp.sqrt(jnp.sum(projected * projected, axis=1, keepdims=True) + 1e-12)
    jitter_key = jax.random.fold_in(key, 103)
    cosine_key = jax.random.fold_in(key, 104)
    scale_key = jax.random.fold_in(key, 105)
    jitter = jax.random.normal(jitter_key, (B, D), jnp.float32)
    cosine = jax.random.uniform(cosine_key, (B, 1), jnp.float32, 0.05, 0.45)
    row_scale = jnp.exp(jax.random.uniform(scale_key, (B, 1), jnp.float32, math.log(0.5), math.log(2.0)))
    jitter = jitter - direction * jnp.sum(jitter * direction, axis=1, keepdims=True)
    jitter = jitter / jnp.sqrt(jnp.sum(jitter * jitter, axis=1, keepdims=True) + 1e-12)
    image_rows = row_scale * (cosine * direction + jnp.sqrt(1.0 - cosine * cosine) * jitter)
    image_bound = 18.0 / math.sqrt(D)
    return jnp.clip(image_rows, -image_bound, image_bound).astype(jnp.bfloat16)


def setup_inputs(seed: int = 0) -> dict:
    key_list = jax.random.split(jax.random.key(seed), 6)
    return {
        "image_embed": draw_image_embed(jax.random.fold_in(key_list[5], 71), 0),
        "text_feature": draw_text_feature(jax.random.fold_in(key_list[5], 71), 0),
        "text_head": draw_text_head(jax.random.fold_in(key_list[5], 71), 0),
        "log_scale": jnp.clip(jax.random.uniform(key_list[3], (1,), jnp.float32, 4.0, 4.8), 4.0, 4.8),
        "bias": jnp.clip(jax.random.uniform(key_list[4], (1,), jnp.float32, -10.0, -6.0), -10.0, -6.0),
    }


EPSILON = 1e-06

def normalized(values):
    widened = values.astype(jnp.float32)
    length = jnp.sqrt(lax.optimization_barrier(jnp.sum(widened * widened, axis=-1, keepdims=True)) + EPSILON)
    return (widened / length, length)

def reference(image_embed, text_feature, text_head, log_scale, bias):
    all_rows = TOK_DEV * N_GRP * N_BLK
    block_rows = all_rows // N_BLK
    image_dir, image_len = normalized(image_embed)
    image_low = image_dir.astype(jnp.bfloat16)
    projected = jnp.dot(text_feature, text_head, preferred_element_type=jnp.float32)
    text_dir, text_len = normalized(projected)
    text_low = text_dir.astype(jnp.bfloat16)
    factor = jnp.exp(log_scale[0])
    offset = bias[0]
    columns = jnp.arange(all_rows, dtype=jnp.int32)

    def visit_block(text_acc, counter):
        first_row = counter * block_rows
        chosen = lax.dynamic_slice_in_dim(image_low, first_row, block_rows, 0)
        logits = factor * lax.dot_general(chosen, text_low, (((1,), (1,)), ((), ())), preferred_element_type=jnp.float32) + offset
        row_ids = first_row + jnp.arange(block_rows, dtype=jnp.int32)
        matched = (row_ids[:, None] == columns[None, :]).astype(jnp.float32)
        weights = (factor * (jax.nn.sigmoid(logits) - matched)).astype(jnp.bfloat16)
        image_part = jnp.dot(weights, text_low, preferred_element_type=jnp.float32)
        text_acc = text_acc + lax.dot_general(weights, chosen, (((0,), (0,)), ((), ())), preferred_element_type=jnp.float32)
        return (text_acc, image_part)
    text_sum, image_parts = lax.scan(visit_block, jnp.zeros((all_rows, D), jnp.float32), jnp.arange(N_BLK, dtype=jnp.int32))
    image_sum = image_parts.reshape(all_rows, D)
    grad_image = ((image_sum - image_dir * lax.optimization_barrier(jnp.sum(image_dir * image_sum, axis=-1, keepdims=True))) / image_len).astype(jnp.bfloat16)
    proj_grad = ((text_sum - text_dir * lax.optimization_barrier(jnp.sum(text_dir * text_sum, axis=-1, keepdims=True))) / text_len).astype(jnp.bfloat16)
    grad_text = lax.dot_general(proj_grad, text_head, (((1,), (1,)), ((), ())), preferred_element_type=jnp.float32).astype(jnp.bfloat16)
    grad_head = lax.dot_general(text_feature, proj_grad, (((0,), (0,)), ((), ())), preferred_element_type=jnp.float32)
    return (grad_image, grad_text, grad_head)
```

```python
import jax
import jax.numpy as jnp
from jax import lax
from jax.experimental import pallas as pl
from jax.experimental.pallas import tpu as pltpu
from jax.sharding import PartitionSpec as P

MESH = pl.DeviceIdType.MESH
EPSILON = 1e-06
F32 = jnp.float32
BF16 = jnp.bfloat16
D = 1152
ROWS = 32
HALF = 16
NX, NY, NZ, NK = 4, 4, 8, 2
ALL = 512
COLS = D // NZ
SLICE = 18


def place():
    grp = lax.axis_index("grp")
    blk = lax.axis_index("blk")
    return blk % 4, (grp // 2) * 2 + (blk // 4) % 2, blk // 8, grp % 2


def device(x, y, z, k):
    return ((y // 2) * 2 + k, z * 8 + (y % 2) * 4 + x)


def rows(start, count):
    return pl.ds(start, count)


def kernel(
    scale_ref, bias_ref, image_ref, text_ref, fsel_ref, head_hbm,
    gi_ref, gt_ref, gh_ref,
    head, img, txt, wt, tp, ip, tpd, rz, iay, iax, ibx, iby,
    tdir, pall, fall, hp, hm, hl, rm, rl, sm, sl, qm, ql,
    head_sem, s_img, r_img, s_z, r_z, s_k, r_k, s_f, r_f, s_rs, r_rs, s_ir, r_ir,
    s_p, r_p, s_h, r_h, s_q, r_q,
):
    x, y, z, k = place()

    def at(dx=0, dy=0, dz=0, dk=0):
        return device((x + dx) % NX, (y + dy) % NY, (z + dz) % NZ, (k + dk) % NK)

    sent = []

    def send(src, dst, ssem, rsem, where):
        copy = pltpu.make_async_remote_copy(
            src_ref=src, dst_ref=dst, send_sem=ssem, recv_sem=rsem,
            device_id=where, device_id_type=MESH,
        )
        copy.start()
        sent.append(copy)
        return copy

    load = pltpu.make_async_copy(head_hbm, head, head_sem)
    load.start()

    barrier = pltpu.get_barrier_semaphore()
    partners = (
        [dict(dx=i) for i in (1, 2, 3)]
        + [dict(dy=i) for i in (1, 2, 3)]
        + [dict(dz=i) for i in range(1, 8)]
        + [dict(dy=i, dk=1) for i in range(4)]
        + [dict(dx=i, dk=1) for i in (1, 2, 3)]
    )
    for p in partners:
        pl.semaphore_signal(barrier, inc=1, device_id=at(**p), device_id_type=MESH)

    wide = image_ref[...].astype(F32)
    image_len = jnp.sqrt(jnp.sum(wide * wide, axis=-1, keepdims=True) + EPSILON)
    low = (wide / image_len).astype(BF16)
    img[rows(0, HALF), :] = low[:HALF]
    img[rows(256, HALF), :] = low[HALF:]

    pl.semaphore_wait(barrier, len(partners))

    ca, cb = {}, {}

    def send_a(dx, dy, sx):
        src = img.at[rows(sx * HALF, HALF), :]
        tx, ty = dx, dy
        slot = ty * 4 + tx
        return src, img.at[rows(slot * HALF, HALF), :], slot

    def ship_a(tx, ty, sx, where):
        src = img.at[rows(sx * HALF, HALF), :]
        slot = ty * 4 + tx
        ca[(tx, ty)] = send(src, img.at[rows(slot * HALF, HALF), :],
                            s_img.at[slot], r_img.at[slot], where)

    def ship_b(tx, ty, sy, where):
        src = img.at[rows(256 + sy * HALF, HALF), :]
        slot = tx * 4 + ty
        cb[(tx, ty)] = send(src, img.at[rows(256 + slot * HALF, HALF), :],
                            s_img.at[16 + slot], r_img.at[16 + slot], where)

    order = (1, 3, 2)
    for i in order:
        ship_a(4 - i, 0, 0, at(dx=i))
        ship_b(0, 4 - i, 0, at(dy=i))
    for i in order:
        ship_a(0, 4 - i, 0, at(dy=i))
        ship_b(4 - i, 0, 0, at(dx=i))

    fall[0] = fsel_ref[k * 4 + x]
    cf = {}
    for dk in range(2):
        for dx in range(4):
            if dk == 0 and dx == 0:
                continue
            slot = ((4 - dx) % 4) + 4 * dk
            cf[slot] = send(fsel_ref.at[((k + dk) % 2) * 4 + (x + dx) % 4], fall.at[slot],
                            s_f.at[slot], r_f.at[slot], at(dx=dx, dk=dk))

    load.wait()
    projected = jnp.dot(text_ref[...], head[...], preferred_element_type=F32)
    text_len = jnp.sqrt(jnp.sum(projected * projected, axis=-1, keepdims=True) + EPSILON)
    text_dir = projected / text_len
    tdir[...] = text_dir
    txt[rows(0, ROWS), :] = text_dir.astype(BF16)

    cz = {}

    def ship_z(sign, step, half):
        src_slot = ((8 - (step - 1)) % 8) if sign > 0 else step - 1
        dst_slot = (8 - step) if sign > 0 else step
        n = ((0 if sign > 0 else 4) + step - 1) * 2 + half
        cz[(sign, step, half)] = send(
            txt.at[rows(src_slot * ROWS + half * HALF, HALF), :],
            txt.at[rows(dst_slot * ROWS + half * HALF, HALF), :],
            s_z.at[n], r_z.at[n], at(dz=sign))

    ck = {}

    def ship_k(slot):
        ck[slot] = send(txt.at[rows(slot * ROWS, ROWS), :], txt.at[rows(256 + slot * ROWS, ROWS), :],
                        s_k.at[slot], r_k.at[slot], at(dk=1))

    for half in range(2):
        ship_z(1, 1, half)
        ship_z(-1, 1, half)
    ship_k(0)

    def forward_image(i):
        ca[(i, 0)].wait_recv()
        for j in order:
            ship_a(i, 4 - j, i, at(dy=j))
        cb[(0, i)].wait_recv()
        for j in order:
            ship_b(4 - j, i, i, at(dx=j))

    forward_image(3)
    forward_image(1)
    for step in (1, 2, 3):
        for half in range(2):
            cz[(1, step, half)].wait_recv()
            if step < 3 or half == 0:
                ship_z(1, step + 1, half)
            cz[(-1, step, half)].wait_recv()
            if step < 3 or half == 1:
                ship_z(-1, step + 1, half)
        ship_k(8 - step)
        ship_k(step)
        if step == 1:
            forward_image(2)
    cz[(1, 4, 0)].wait_recv()
    cz[(-1, 4, 1)].wait_recv()
    ship_k(4)

    for i in (0, 1, 2, 3):
        for j in (1, 2, 3):
            ca[(i, j)].wait_recv()
            cb[(j, i)].wait_recv()
    for slot in range(8):
        ck[slot].wait_recv()

    factor = jnp.exp(jnp.full((1, 1), scale_ref[0], F32))
    offset = bias_ref[0]

    def tile(i):
        part = rows(pl.multiple_of(i * 128, 128), 128)
        logits = factor * lax.dot_general(
            txt[part, :], img[...], (((1,), (1,)), ((), ())), preferred_element_type=F32) + offset
        row = lax.broadcasted_iota(jnp.int32, (128, ALL), 0) + i * 128
        col = lax.broadcasted_iota(jnp.int32, (128, ALL), 1)
        want = jnp.where(row < HALF, row, row + 240)
        matched = jnp.where((row < ROWS) & (col == want), 1.0, 0.0).astype(F32)
        weights = (factor * (jax.nn.sigmoid(logits) - matched)).astype(BF16)
        wt[part, :] = weights
        tp[part, :] = jnp.dot(weights, img[...], preferred_element_type=F32).astype(BF16)

    pl.loop(2, 4)(tile)
    exchange = send(tp.at[rows(256, 256), :], tpd, s_k.at[8], r_k.at[8], at(dk=1))
    pl.loop(0, 2)(tile)
    exchange.wait_recv()

    def join(i):
        part = rows(pl.multiple_of(i * ROWS, ROWS), ROWS)
        tp[part, :] = (tp[part, :].astype(F32) + tpd[part, :].astype(F32)).astype(BF16)

    pl.loop(0, 8)(join)

    cr = {}

    def rz_slot(sign, dist, half):
        return ((0 if sign > 0 else 4) + dist - 1) * 2 + half

    def ship_rs(sign, dist, half):
        slot = dist if sign > 0 else (8 - dist)
        n = rz_slot(sign, dist, half)
        cr[(sign, dist, half)] = send(
            tp.at[rows(slot * ROWS + half * HALF, HALF), :], rz.at[n], s_rs.at[n], r_rs.at[n], at(dz=sign))

    def take_rs(sign, dist, half):
        cr[(sign, dist, half)].wait_recv()
        slot = (dist - 1) if sign > 0 else (9 - dist)
        part = rows(slot * ROWS + half * HALF, HALF)
        tp[part, :] = (tp[part, :].astype(F32) + rz[rz_slot(sign, dist, half)].astype(F32)).astype(BF16)
        ship_rs(sign, dist - 1, half)

    ship_rs(1, 4, 0)
    ship_rs(-1, 4, 1)
    ship_rs(1, 3, 1)
    ship_rs(-1, 3, 0)

    def image_tile(i):
        part = rows(pl.multiple_of(i * 128, 128), 128)
        ip[part, :] = lax.dot_general(
            wt[:, part], txt[...], (((0,), (0,)), ((), ())), preferred_element_type=F32).astype(BF16)

    ci = {}

    def ship_ir(name, dist, src, dst, n, where):
        ci[(name, dist)] = send(src, dst, s_ir.at[n], r_ir.at[n], where)

    pl.loop(0, 2)(image_tile)
    for i in order:
        ship_ir("ay", i, ip.at[rows(i * 64, 64), :], iay.at[i - 1], i - 1, at(dy=i))
    take_rs(1, 4, 0)
    take_rs(-1, 4, 1)
    take_rs(1, 3, 1)
    take_rs(-1, 3, 0)
    pl.loop(2, 4)(image_tile)
    for i in order:
        ship_ir("bx", i, ip.at[rows(256 + i * 64, 64), :], ibx.at[i - 1], 3 + i - 1, at(dx=i))
    take_rs(1, 3, 0)
    take_rs(-1, 3, 1)
    take_rs(1, 2, 1)
    take_rs(-1, 2, 0)

    def fold(base, recv, name):
        for i in order:
            ci[(name, i)].wait_recv()
        for j in range(4):
            part = rows(base + j * HALF, HALF)
            inner = rows(j * HALF, HALF)
            total = ip[part, :].astype(F32)
            for i in range(3):
                total = total + recv[i, inner, :].astype(F32)
            ip[part, :] = total.astype(BF16)

    fold(0, iay, "ay")
    for i in order:
        ship_ir("ax", i, ip.at[rows(i * HALF, HALF), :], iax.at[i - 1], 6 + i - 1, at(dx=i))
    take_rs(1, 2, 0)
    take_rs(-1, 2, 1)
    fold(256, ibx, "bx")
    for i in order:
        ship_ir("by", i, ip.at[rows(256 + i * HALF, HALF), :], iby.at[i - 1], 9 + i - 1, at(dy=i))

    for sign in (1, -1):
        for half in range(2):
            cr[(sign, 1, half)].wait_recv()
    halves = []
    for half in range(2):
        total = tp[rows(half * HALF, HALF), :].astype(F32)
        total = total + rz[rz_slot(1, 1, half)].astype(F32) + rz[rz_slot(-1, 1, half)].astype(F32)
        halves.append(total)
    text_sum = jnp.concatenate(halves, axis=0)
    text_dir = tdir[...]
    proj_grad = (
        (text_sum - text_dir * jnp.sum(text_dir * text_sum, axis=-1, keepdims=True)) / text_len
    ).astype(BF16)
    pall[0] = proj_grad

    cp = {}
    for dx in order:
        slot = 4 - dx
        cp[slot] = send(pall.at[0], pall.at[slot], s_p.at[slot], r_p.at[slot], at(dx=dx))
    cp[4] = send(pall.at[0], pall.at[4], s_p.at[4], r_p.at[4], at(dk=1))

    gt_ref[...] = lax.dot_general(
        proj_grad, head[...], (((1,), (1,)), ((), ())), preferred_element_type=F32).astype(BF16)

    for slot in (1, 3, 2):
        cp[slot].wait_recv()
        cp[4 + slot] = send(pall.at[slot], pall.at[4 + slot], s_p.at[4 + slot], r_p.at[4 + slot], at(dk=1))
    for slot in range(4, 8):
        cp[slot].wait_recv()
    for slot in range(1, 8):
        cf[slot].wait_recv()

    hp[...] = lax.dot_general(
        fall[...].reshape(256, COLS), pall[...].reshape(256, D), (((0,), (0,)), ((), ())),
        preferred_element_type=F32)
    for s in range(NZ):
        part = hp[rows(s * SLICE, SLICE), :]
        hm[s] = part[:HALF].astype(BF16)
        hl[s] = part[HALF:].astype(BF16)
    ch = {}
    for dz in (1, 7, 2, 6, 3, 5, 4):
        dest = (z + dz) % NZ
        ch[dz] = (
            send(hm.at[dest], rm.at[dz], s_h.at[dz], r_h.at[dz], at(dz=dz)),
            send(hl.at[dest], rl.at[dz], s_h.at[8 + dz], r_h.at[8 + dz], at(dz=dz)),
        )

    for name in ("ax", "by"):
        for i in order:
            ci[(name, i)].wait_recv()
    total_a = ip[rows(0, HALF), :].astype(F32)
    total_b = ip[rows(256, HALF), :].astype(F32)
    for i in range(3):
        total_a = total_a + iax[i].astype(F32)
        total_b = total_b + iby[i].astype(F32)
    image_sum = jnp.concatenate([total_a, total_b], axis=0)
    wide = image_ref[...].astype(F32)
    image_len = jnp.sqrt(jnp.sum(wide * wide, axis=-1, keepdims=True) + EPSILON)
    image_dir = wide / image_len
    gi_ref[...] = (
        (image_sum - image_dir * jnp.sum(image_dir * image_sum, axis=-1, keepdims=True)) / image_len
    ).astype(BF16)

    main = hm[z].astype(F32)
    left = hl[z].astype(F32)
    for dz in (1, 7, 2, 6, 3, 5, 4):
        for copy in ch[dz]:
            copy.wait_recv()
        main = main + rm[dz].astype(F32)
        left = left + rl[dz].astype(F32)
    sm[...] = main.astype(BF16)
    sl[...] = left.astype(BF16)

    y_lo = y % 2

    def final(target_y, target_k, slot):
        return (
            pltpu.make_async_remote_copy(
                src_ref=sm, dst_ref=qm.at[slot], send_sem=s_q.at[target_y // 2 * 2 + target_k],
                recv_sem=r_q.at[slot], device_id=device(x, target_y, z, target_k), device_id_type=MESH),
            pltpu.make_async_remote_copy(
                src_ref=sl, dst_ref=ql.at[slot], send_sem=s_q.at[4 + target_y // 2 * 2 + target_k],
                recv_sem=r_q.at[4 + slot], device_id=device(x, target_y, z, target_k), device_id_type=MESH),
        )

    for h in range(2):
        for tk in range(2):
            ty = k + 2 * h
            own = (ty == y) & (tk == k)

            @pl.when(jnp.logical_not(own))
            def _():
                for copy in final(ty, tk, y):
                    copy.start()

            @pl.when(own)
            def _():
                qm[y] = sm[...]
                ql[y] = sl[...]

    for sy in range(4):
        @pl.when(jnp.logical_not((sy == y) & (k == y_lo)))
        def _():
            for copy in final(y, k, sy):
                copy.wait_recv()

    main = qm[0].astype(F32)
    left = ql[0].astype(F32)
    for sy in range(1, 4):
        main = main + qm[sy].astype(F32)
        left = left + ql[sy].astype(F32)
    gh_ref[pl.ds(0, HALF), :] = main
    gh_ref[pl.ds(HALF, 2), :] = left

    for copy in sent:
        copy.wait_send()
    for h in range(2):
        for tk in range(2):
            ty = k + 2 * h

            @pl.when(jnp.logical_not((ty == y) & (tk == k)))
            def _():
                for copy in final(ty, tk, y):
                    copy.wait_send()


def local(image_embed, text_feature, text_head, log_scale, bias):
    fsel = text_feature.reshape(ROWS, NZ, 8, SLICE).transpose(2, 0, 1, 3).reshape(8, ROWS, COLS)
    vmem = pl.BlockSpec(memory_space=pltpu.VMEM)
    smem = pl.BlockSpec(memory_space=pltpu.SMEM)
    dma = pltpu.SemaphoreType.DMA
    V = pltpu.VMEM
    return pl.pallas_call(
        kernel,
        out_shape=(
            jax.ShapeDtypeStruct((ROWS, D), BF16),
            jax.ShapeDtypeStruct((ROWS, D), BF16),
            jax.ShapeDtypeStruct((SLICE, D), F32),
        ),
        in_specs=[smem, smem, vmem, vmem, vmem, pl.BlockSpec(memory_space=pl.ANY)],
        out_specs=(vmem, vmem, vmem),
        scratch_shapes=[
            V((D, D), BF16),
            V((ALL, D), BF16),
            V((ALL, D), BF16),
            V((ALL, ALL), BF16),
            V((ALL, D), BF16),
            V((ALL, D), BF16),
            V((256, D), BF16),
            V((16, HALF, D), BF16),
            V((3, 64, D), BF16),
            V((3, HALF, D), BF16),
            V((3, 64, D), BF16),
            V((3, HALF, D), BF16),
            V((ROWS, D), F32),
            V((8, ROWS, D), BF16),
            V((8, ROWS, COLS), BF16),
            V((COLS, D), F32),
            V((NZ, HALF, D), BF16),
            V((NZ, 2, D), BF16),
            V((NZ, HALF, D), BF16),
            V((NZ, 2, D), BF16),
            V((HALF, D), BF16),
            V((2, D), BF16),
            V((4, HALF, D), BF16),
            V((4, 2, D), BF16),
            dma,
            dma((32,)), dma((32,)),
            dma((16,)), dma((16,)),
            dma((9,)), dma((9,)),
            dma((8,)), dma((8,)),
            dma((16,)), dma((16,)),
            dma((12,)), dma((12,)),
            dma((8,)), dma((8,)),
            dma((16,)), dma((16,)),
            dma((8,)), dma((8,)),
        ],
        compiler_params=pltpu.CompilerParams(
            collective_id=0, has_side_effects=True, vmem_limit_bytes=48 * 2**20),
        name="contrastive",
    )(log_scale, bias, image_embed, text_feature, fsel, text_head)


def solution(mesh):
    both = P(("grp", "blk"), None)
    return jax.shard_map(
        local,
        mesh=mesh,
        in_specs=(both, both, P(), P(), P()),
        out_specs=(both, both, P("blk", None)),
        check_vma=False,
    )
```

```python
import jax
import jax.numpy as jnp
from jax import lax
from jax.experimental import pallas as pl
from jax.experimental.pallas import tpu as pltpu
from jax.sharding import PartitionSpec as P

MESH = pl.DeviceIdType.MESH
EPSILON = 1e-06
F32 = jnp.float32
BF16 = jnp.bfloat16
D = 1152
ROWS = 32
HALF = 16
NX, NY, NZ, NK = 4, 4, 8, 2
ALL = 512
COLS = D // NZ
SLICE = 18


def place():
    grp = lax.axis_index("grp")
    blk = lax.axis_index("blk")
    return blk % 4, (grp // 2) * 2 + (blk // 4) % 2, blk // 8, grp % 2


def device(x, y, z, k):
    return ((y // 2) * 2 + k, z * 8 + (y % 2) * 4 + x)


GROUPS = ((0, 1), (2, 7), (3, 6), (4, 5))
TEXT_ROW = {s: g * 128 + j * ROWS for g, pair in enumerate(GROUPS) for j, s in enumerate(pair)}
CHUNKS = ((0, 640), (640, 512))


def rows(start, count):
    return pl.ds(start, count)


def kernel(
    scalar_ref, image_hbm, text_hbm, head_hbm,
    gi_hbm, gt_hbm, gh_hbm,
    gi_ref, gt_ref, gh_ref, image_ref, text_ref, fsel_ref, head, img, txt, wt, tp, ip, tpd, rz, iay, iax, ibx, iby,
    tdir, pall, fall, hp, hm, hl, rm, rl, sm, sl, qm, ql,
    in_sem, out_sem, s_img, r_img, s_z, r_z, s_k, r_k, s_f, r_f, s_rs, r_rs, s_ir, r_ir,
    s_p, r_p, s_h, r_h, s_q, r_q,
):
    x, y, z, k = place()

    def at(dx=0, dy=0, dz=0, dk=0):
        return device((x + dx) % NX, (y + dy) % NY, (z + dz) % NZ, (k + dk) % NK)

    sent = []

    def send(src, dst, ssem, rsem, where):
        copy = pltpu.make_async_remote_copy(
            src_ref=src, dst_ref=dst, send_sem=ssem, recv_sem=rsem,
            device_id=where, device_id_type=MESH,
        )
        copy.start()
        sent.append(copy)
        return copy

    loads = []
    for n, (src, dst) in enumerate((
        (image_hbm, image_ref), (head_hbm, head), (text_hbm, text_ref),
    )):
        loads.append(pltpu.make_async_copy(src, dst, in_sem.at[n]))
        loads[n].start()

    barrier = pltpu.get_barrier_semaphore()
    partners = (
        [dict(dx=i) for i in (1, 2, 3)]
        + [dict(dy=i) for i in (1, 2, 3)]
        + [dict(dz=1), dict(dz=7), dict(dk=1)]
    )
    for p in partners:
        pl.semaphore_signal(barrier, inc=1, device_id=at(**p), device_id_type=MESH)

    loads[0].wait()
    wide = image_ref[...].astype(F32)
    image_len = jnp.sqrt(jnp.sum(wide * wide, axis=-1, keepdims=True) + EPSILON)
    low = (wide / image_len).astype(BF16)
    img[rows(0, HALF), :] = low[:HALF]
    img[rows(256, HALF), :] = low[HALF:]

    pl.semaphore_wait(barrier, len(partners))

    ca, cb = {}, {}

    def send_a(dx, dy, sx):
        src = img.at[rows(sx * HALF, HALF), :]
        tx, ty = dx, dy
        slot = ty * 4 + tx
        return src, img.at[rows(slot * HALF, HALF), :], slot

    def ship_a(tx, ty, sx, where):
        src = img.at[rows(sx * HALF, HALF), :]
        slot = ty * 4 + tx
        ca[(tx, ty)] = send(src, img.at[rows(slot * HALF, HALF), :],
                            s_img.at[slot], r_img.at[slot], where)

    def ship_b(tx, ty, sy, where):
        src = img.at[rows(256 + sy * HALF, HALF), :]
        slot = tx * 4 + ty
        cb[(tx, ty)] = send(src, img.at[rows(256 + slot * HALF, HALF), :],
                            s_img.at[16 + slot], r_img.at[16 + slot], where)

    order = (1, 3, 2)
    for i in order:
        ship_a(4 - i, 0, 0, at(dx=i))
        ship_b(0, 4 - i, 0, at(dy=i))
    for i in order:
        ship_a(0, 4 - i, 0, at(dy=i))
        ship_b(4 - i, 0, 0, at(dx=i))

    loads[1].wait()
    loads[2].wait()
    projected = jnp.dot(text_ref[...], head[...], preferred_element_type=F32)
    text_len = jnp.sqrt(jnp.sum(projected * projected, axis=-1, keepdims=True) + EPSILON)
    text_dir = projected / text_len
    tdir[...] = text_dir
    txt[rows(0, ROWS), :] = text_dir.astype(BF16)

    cz = {}

    def ship_zc(sign, step, half, c):
        src_slot = ((8 - (step - 1)) % 8) if sign > 0 else step - 1
        dst_slot = (8 - step) if sign > 0 else step
        n = (((0 if sign > 0 else 4) + step - 1) * 2 + half) * 2 + c
        cz[(sign, step, half, c)] = send(
            txt.at[rows(TEXT_ROW[src_slot] + half * HALF, HALF), pl.ds(*CHUNKS[c])],
            txt.at[rows(TEXT_ROW[dst_slot] + half * HALF, HALF), pl.ds(*CHUNKS[c])],
            s_z.at[n], r_z.at[n], at(dz=sign))

    ck = {}

    def ship_k(slot):
        ck[slot] = send(txt.at[rows(TEXT_ROW[slot], ROWS), :], txt.at[rows(TEXT_ROW[slot] + 64, ROWS), :],
                        s_k.at[slot], r_k.at[slot], at(dk=1))

    for half in range(2):
        for c in range(2):
            ship_zc(1, 1, half, c)
            ship_zc(-1, 1, half, c)
    ship_k(0)

    def forward_image(i):
        ca[(i, 0)].wait_recv()
        for j in order:
            ship_a(i, 4 - j, i, at(dy=j))
        cb[(0, i)].wait_recv()
        for j in order:
            ship_b(4 - j, i, i, at(dx=j))

    column = lax.broadcasted_iota(jnp.int32, (1, COLS), 1)
    source = column
    for n in range(1, NZ):
        source = source + jnp.where(column >= n * SLICE, COLS - SLICE, 0)
    entry = lax.broadcasted_iota(jnp.int32, (D, COLS), 0)

    def select(q):
        chosen = jnp.where(entry == source + q * SLICE, 1.0, 0.0).astype(BF16)
        fsel_ref[q] = jnp.dot(text_ref[...], chosen, preferred_element_type=F32).astype(BF16)

    forward_image(3)
    forward_image(1)
    for step in (1, 2, 3):
        for half in range(2):
            for c in range(2):
                cz[(1, step, half, c)].wait_recv()
                if step < 3 or half == 0:
                    ship_zc(1, step + 1, half, c)
                cz[(-1, step, half, c)].wait_recv()
                if step < 3 or half == 1:
                    ship_zc(-1, step + 1, half, c)
        ship_k(8 - step)
        ship_k(step)
        if step == 1:
            forward_image(2)
            pl.loop(0, 4)(select)
        if step == 2:
            pl.loop(4, 8)(select)
    for c in range(2):
        cz[(1, 4, 0, c)].wait_recv()
        cz[(-1, 4, 1, c)].wait_recv()
    ship_k(4)

    for i in (0, 1, 2, 3):
        for j in (1, 2, 3):
            ca[(i, j)].wait_recv()
            cb[(j, i)].wait_recv()
    for slot in range(8):
        ck[slot].wait_recv()

    factor = jnp.exp(jnp.full((1, 1), scalar_ref[0], F32))
    offset = scalar_ref[1]

    def tile(i):
        part = rows(i * 128, 128)
        logits = factor * lax.dot_general(
            txt[part, :], img[...], (((1,), (1,)), ((), ())), preferred_element_type=F32) + offset
        prob = jax.nn.sigmoid(logits)
        if i == 0:
            row = lax.broadcasted_iota(jnp.int32, (128, ALL), 0)
            col = lax.broadcasted_iota(jnp.int32, (128, ALL), 1)
            want = jnp.where(row < HALF, row, row + 240)
            prob = prob - jnp.where((row < ROWS) & (col == want), 1.0, 0.0).astype(F32)
        weights = (factor * prob).astype(BF16)
        wt[part, :] = weights
        tp[part, :] = jnp.dot(weights, img[...], preferred_element_type=F32).astype(BF16)

    ce = {}

    def give(g):
        tile(g)
        ce[g] = send(tp.at[rows(g * 128 + 64, 64), :], tpd.at[g], s_k.at[8 + g], r_k.at[8 + g], at(dk=1))

    def join(g):
        ce[g].wait_recv()
        for j in range(4):
            part = rows(g * 128 + j * HALF, HALF)
            tp[part, :] = (tp[part, :].astype(F32) + tpd[g, rows(j * HALF, HALF), :].astype(F32)).astype(BF16)

    cr = {}

    def rz_slot(sign, dist, half):
        return ((0 if sign > 0 else 4) + dist - 1) * 2 + half

    def ship_rs(sign, dist, half, c):
        slot = dist if sign > 0 else (8 - dist)
        n = rz_slot(sign, dist, half)
        cols = pl.ds(*CHUNKS[c])
        cr[(sign, dist, half, c)] = send(
            tp.at[rows(TEXT_ROW[slot] + half * HALF, HALF), cols], rz.at[n, :, cols],
            s_rs.at[n * 2 + c], r_rs.at[n * 2 + c], at(dz=sign))

    def take_rs(sign, dist, half):
        slot = (dist - 1) if sign > 0 else (9 - dist)
        part = rows(TEXT_ROW[slot] + half * HALF, HALF)
        for c in range(2):
            cols = pl.ds(*CHUNKS[c])
            cr[(sign, dist, half, c)].wait_recv()
            tp[part, cols] = (
                tp[part, cols].astype(F32) + rz[rz_slot(sign, dist, half), :, cols].astype(F32)
            ).astype(BF16)
            ship_rs(sign, dist - 1, half, c)

    def image_tile(i):
        part = rows(i * 128, 128)
        ip[part, :] = lax.dot_general(
            wt[:, part], txt[...], (((0,), (0,)), ((), ())), preferred_element_type=F32).astype(BF16)

    ci = {}

    def ship_ir(name, dist, src, dst, n, where):
        ci[(name, dist)] = send(src, dst, s_ir.at[n], r_ir.at[n], where)

    give(3)
    give(2)
    join(3)
    for c in range(2):
        ship_rs(1, 4, 0, c)
        ship_rs(-1, 4, 1, c)
        ship_rs(-1, 3, 0, c)
    join(2)
    for c in range(2):
        ship_rs(1, 3, 1, c)
    give(1)
    give(0)
    join(1)
    take_rs(1, 4, 0)
    take_rs(-1, 4, 1)
    take_rs(1, 3, 1)
    take_rs(-1, 3, 0)
    join(0)

    fall[0] = fsel_ref[k * 4 + x]
    cf = {}
    for dk in range(2):
        for dx in range(4):
            if dk == 0 and dx == 0:
                continue
            slot = ((4 - dx) % 4) + 4 * dk
            cf[slot] = send(fsel_ref.at[((k + dk) % 2) * 4 + (x + dx) % 4], fall.at[slot],
                            s_f.at[slot], r_f.at[slot], at(dx=dx, dk=dk))

    image_tile(0)
    image_tile(1)
    for i in order:
        ship_ir("ay", i, ip.at[rows(i * 64, 64), :], iay.at[i - 1], i - 1, at(dy=i))
    take_rs(1, 3, 0)
    take_rs(-1, 3, 1)
    take_rs(1, 2, 1)
    take_rs(-1, 2, 0)
    image_tile(2)
    image_tile(3)
    for i in order:
        ship_ir("bx", i, ip.at[rows(256 + i * 64, 64), :], ibx.at[i - 1], 3 + i - 1, at(dx=i))

    def fold(base, recv, name):
        for i in order:
            ci[(name, i)].wait_recv()
        for j in range(4):
            part = rows(base + j * HALF, HALF)
            inner = rows(j * HALF, HALF)
            total = ip[part, :].astype(F32)
            for i in range(3):
                total = total + recv[i, inner, :].astype(F32)
            ip[part, :] = total.astype(BF16)

    take_rs(1, 2, 0)
    take_rs(-1, 2, 1)

    for half in range(2):
        for sign in (1, -1):
            for c in range(2):
                cr[(sign, 1, half, c)].wait_recv()
    halves = []
    for half in range(2):
        total = tp[rows(half * HALF, HALF), :].astype(F32)
        total = total + rz[rz_slot(1, 1, half)].astype(F32) + rz[rz_slot(-1, 1, half)].astype(F32)
        halves.append(total)
    text_sum = jnp.concatenate(halves, axis=0)
    text_dir = tdir[...]
    proj_grad = (
        (text_sum - text_dir * jnp.sum(text_dir * text_sum, axis=-1, keepdims=True)) / text_len
    ).astype(BF16)
    pall[0] = proj_grad

    cp = {}
    for dx in order:
        slot = 4 - dx
        cp[slot] = send(pall.at[0], pall.at[slot], s_p.at[slot], r_p.at[slot], at(dx=dx))
    cp[4] = send(pall.at[0], pall.at[4], s_p.at[4], r_p.at[4], at(dk=1))

    gt_ref[...] = lax.dot_general(
        proj_grad, head[...], (((1,), (1,)), ((), ())), preferred_element_type=F32).astype(BF16)

    outs = [
        pltpu.make_async_copy(src, dst, out_sem.at[n])
        for n, (src, dst) in enumerate(((gi_ref, gi_hbm), (gt_ref, gt_hbm), (gh_ref, gh_hbm)))
    ]
    outs[1].start()
    fold(0, iay, "ay")
    for i in order:
        ship_ir("ax", i, ip.at[rows(i * HALF, HALF), :], iax.at[i - 1], 6 + i - 1, at(dx=i))
    fold(256, ibx, "bx")
    for i in order:
        ship_ir("by", i, ip.at[rows(256 + i * HALF, HALF), :], iby.at[i - 1], 9 + i - 1, at(dy=i))

    for slot in (1, 3, 2):
        cp[slot].wait_recv()
        cp[4 + slot] = send(pall.at[slot], pall.at[4 + slot], s_p.at[4 + slot], r_p.at[4 + slot], at(dk=1))
    for slot in range(4, 8):
        cp[slot].wait_recv()
    for slot in range(1, 8):
        cf[slot].wait_recv()

    hp[...] = lax.dot_general(
        fall[...].reshape(256, COLS), pall[...].reshape(256, D), (((0,), (0,)), ((), ())),
        preferred_element_type=F32)
    for s in range(NZ):
        part = hp[rows(s * SLICE, SLICE), :]
        hm[s] = part[:HALF].astype(BF16)
        hl[s] = part[HALF:].astype(BF16)
    ch = {}
    for dz in (1, 7, 2, 6, 3, 5, 4):
        dest = (z + dz) % NZ
        ch[dz] = (
            send(hm.at[dest], rm.at[dz], s_h.at[dz], r_h.at[dz], at(dz=dz)),
            send(hl.at[dest], rl.at[dz], s_h.at[8 + dz], r_h.at[8 + dz], at(dz=dz)),
        )

    for name in ("ax", "by"):
        for i in order:
            ci[(name, i)].wait_recv()
    total_a = ip[rows(0, HALF), :].astype(F32)
    total_b = ip[rows(256, HALF), :].astype(F32)
    for i in range(3):
        total_a = total_a + iax[i].astype(F32)
        total_b = total_b + iby[i].astype(F32)
    image_sum = jnp.concatenate([total_a, total_b], axis=0)
    wide = image_ref[...].astype(F32)
    image_len = jnp.sqrt(jnp.sum(wide * wide, axis=-1, keepdims=True) + EPSILON)
    image_dir = wide / image_len
    gi_ref[...] = (
        (image_sum - image_dir * jnp.sum(image_dir * image_sum, axis=-1, keepdims=True)) / image_len
    ).astype(BF16)

    outs[0].start()
    main = hm[z].astype(F32)
    left = hl[z].astype(F32)
    for dz in (1, 7, 2, 6, 3, 5, 4):
        for copy in ch[dz]:
            copy.wait_recv()
        main = main + rm[dz].astype(F32)
        left = left + rl[dz].astype(F32)
    sm[...] = main.astype(BF16)
    sl[...] = left.astype(BF16)

    y_lo = y % 2

    def final(target_y, target_k, slot):
        return (
            pltpu.make_async_remote_copy(
                src_ref=sm, dst_ref=qm.at[slot], send_sem=s_q.at[target_y // 2 * 2 + target_k],
                recv_sem=r_q.at[slot], device_id=device(x, target_y, z, target_k), device_id_type=MESH),
            pltpu.make_async_remote_copy(
                src_ref=sl, dst_ref=ql.at[slot], send_sem=s_q.at[4 + target_y // 2 * 2 + target_k],
                recv_sem=r_q.at[4 + slot], device_id=device(x, target_y, z, target_k), device_id_type=MESH),
        )

    for h in range(2):
        for tk in range(2):
            ty = k + 2 * h
            own = (ty == y) & (tk == k)

            @pl.when(jnp.logical_not(own))
            def _():
                for copy in final(ty, tk, y):
                    copy.start()

            @pl.when(own)
            def _():
                qm[y] = sm[...]
                ql[y] = sl[...]

    for sy in range(4):
        @pl.when(jnp.logical_not((sy == y) & (k == y_lo)))
        def _():
            for copy in final(y, k, sy):
                copy.wait_recv()

    main = qm[0].astype(F32)
    left = ql[0].astype(F32)
    for sy in range(1, 4):
        main = main + qm[sy].astype(F32)
        left = left + ql[sy].astype(F32)
    gh_ref[pl.ds(0, HALF), :] = main
    gh_ref[pl.ds(HALF, 2), :] = left
    outs[2].start()

    for copy in sent:
        copy.wait_send()
    for h in range(2):
        for tk in range(2):
            ty = k + 2 * h

            @pl.when(jnp.logical_not((ty == y) & (tk == k)))
            def _():
                for copy in final(ty, tk, y):
                    copy.wait_send()
    for copy in outs:
        copy.wait()


def deliver(gi_in, gt_in, gh_in, gi_out, gt_out, gh_out, gi_ref, gt_ref, gh_ref, in_sem, out_sem):
    first = [
        pltpu.make_async_copy(src, dst, in_sem.at[n])
        for n, (src, dst) in enumerate(((gi_in, gi_ref), (gt_in, gt_ref), (gh_in, gh_ref)))
    ]
    second = [
        pltpu.make_async_copy(src, dst, out_sem.at[n])
        for n, (src, dst) in enumerate(((gi_ref, gi_out), (gt_ref, gt_out), (gh_ref, gh_out)))
    ]
    for copy in first:
        copy.start()
    for n in range(3):
        first[n].wait()
        second[n].start()
    for copy in second:
        copy.wait()


def local(image_embed, text_feature, text_head, log_scale, bias):
    hbm = pl.BlockSpec(memory_space=pltpu.HBM)
    dma = pltpu.SemaphoreType.DMA
    V = pltpu.VMEM
    shapes = (
        jax.ShapeDtypeStruct((ROWS, D), BF16),
        jax.ShapeDtypeStruct((ROWS, D), BF16),
        jax.ShapeDtypeStruct((SLICE, D), F32),
    )
    results = pl.pallas_call(
        kernel,
        out_shape=shapes,
        in_specs=[pl.BlockSpec(memory_space=pltpu.SMEM)] + [hbm] * 3,
        out_specs=(hbm, hbm, hbm),
        scratch_shapes=[
            V((ROWS, D), BF16),
            V((ROWS, D), BF16),
            V((SLICE, D), F32),
            V((ROWS, D), BF16),
            V((ROWS, D), BF16),
            V((8, ROWS, COLS), BF16),
            V((D, D), BF16),
            V((ALL, D), BF16),
            V((ALL, D), BF16),
            V((ALL, ALL), BF16),
            V((ALL, D), BF16),
            V((ALL, D), BF16),
            V((4, 64, D), BF16),
            V((16, HALF, D), BF16),
            V((3, 64, D), BF16),
            V((3, HALF, D), BF16),
            V((3, 64, D), BF16),
            V((3, HALF, D), BF16),
            V((ROWS, D), F32),
            V((8, ROWS, D), BF16),
            V((8, ROWS, COLS), BF16),
            V((COLS, D), F32),
            V((NZ, HALF, D), BF16),
            V((NZ, 2, D), BF16),
            V((NZ, HALF, D), BF16),
            V((NZ, 2, D), BF16),
            V((HALF, D), BF16),
            V((2, D), BF16),
            V((4, HALF, D), BF16),
            V((4, 2, D), BF16),
            dma((3,)), dma((3,)),
            dma((32,)), dma((32,)),
            dma((32,)), dma((32,)),
            dma((12,)), dma((12,)),
            dma((8,)), dma((8,)),
            dma((32,)), dma((32,)),
            dma((12,)), dma((12,)),
            dma((8,)), dma((8,)),
            dma((16,)), dma((16,)),
            dma((8,)), dma((8,)),
        ],
        compiler_params=pltpu.CompilerParams(
            collective_id=0, has_side_effects=True, vmem_limit_bytes=66500000),
        name="contrastive",
    )(jnp.concatenate([log_scale, bias]), image_embed, text_feature, text_head)
    return pl.pallas_call(
        deliver,
        out_shape=shapes,
        in_specs=[hbm] * 3,
        out_specs=(hbm, hbm, hbm),
        scratch_shapes=[
            V((ROWS, D), BF16), V((ROWS, D), BF16), V((SLICE, D), F32), dma((3,)), dma((3,))],
        compiler_params=pltpu.CompilerParams(vmem_limit_bytes=66500000),
        name="deliver",
    )(*results)


def solution(mesh):
    both = P(("grp", "blk"), None)
    return jax.shard_map(
        local,
        mesh=mesh,
        in_specs=(both, both, P(), P(), P()),
        out_specs=(both, both, P("blk", None)),
        check_vma=False,
    )
```

```python
import jax
import jax.numpy as jnp
from jax import lax
from jax.experimental import pallas as pl
from jax.experimental.pallas import tpu as pltpu
from jax.sharding import PartitionSpec as P

MESH = pl.DeviceIdType.MESH
EPSILON = 1e-06
F32 = jnp.float32
BF16 = jnp.bfloat16
D = 1152
ROWS = 32
HALF = 16
NX, NY, NZ, NK = 4, 4, 8, 2
COLS = D // NZ
SLICE = 18


def place():
    grp = lax.axis_index("grp")
    blk = lax.axis_index("blk")
    return blk % 4, (grp // 2) * 2 + (blk // 4) % 2, blk // 8, grp % 2


def device(x, y, z, k):
    return ((y // 2) * 2 + k, z * 8 + (y % 2) * 4 + x)


TEXT_ROW = {s: n * ROWS for n, s in enumerate((0, 1, 7, 2, 6, 3, 5, 4))}
TEXTS = 256
IMAGES = 1024
CHUNKS = ((0, 640), (640, 512))


def rows(start, count):
    return pl.ds(start, count)


def kernel(
    scalar_ref, image_hbm, text_hbm, head_hbm,
    gi_hbm, gt_hbm, gh_hbm,
    gi_ref, gt_ref, gh_ref, image_ref, text_ref, fsel_ref, head, img, txt, wt, tp, ip, rz, iay, iax, ibx, iby,
    ipd, tdir, pall, fall, hp, hm, hl, rm, rl, sm, sl, qm, ql,
    in_sem, out_sem, r_first, r_second, r_pair, r_z, r_f, r_rs, r_rs1, r_ex, r_ir,
    r_p, r_pk, r_hm, r_hl, s_q, r_q, s_all,
):
    x, y, z, k = place()

    def at(dx=0, dy=0, dz=0, dk=0):
        return device((x + dx) % NX, (y + dy) % NY, (z + dz) % NZ, (k + dk) % NK)

    def send(src, dst, group, rsem, where):
        copy = pltpu.make_async_remote_copy(
            src_ref=src, dst_ref=dst, send_sem=s_all.at[group], recv_sem=rsem,
            device_id=where, device_id_type=MESH,
        )
        copy.start()
        return copy

    def wait_all(ref, sem):
        pltpu.make_async_remote_copy(
            src_ref=ref, dst_ref=ref, send_sem=sem, recv_sem=sem,
            device_id=at(dk=1), device_id_type=MESH,
        ).wait_recv()

    loads = []
    for n, (src, dst) in enumerate((
        (image_hbm, image_ref), (head_hbm, head), (text_hbm, text_ref),
    )):
        loads.append(pltpu.make_async_copy(src, dst, in_sem.at[n]))
        loads[n].start()

    barrier = pltpu.get_barrier_semaphore()
    partners = (
        [dict(dx=i) for i in (1, 2, 3)]
        + [dict(dy=i) for i in (1, 2, 3)]
        + [dict(dz=1), dict(dz=7), dict(dk=1)]
    )
    for p in partners:
        pl.semaphore_signal(barrier, inc=1, device_id=at(**p), device_id_type=MESH)

    loads[0].wait()
    wide = image_ref[...].astype(F32)
    image_len = jnp.sqrt(jnp.sum(wide * wide, axis=-1, keepdims=True) + EPSILON)
    low = (wide / image_len).astype(BF16)
    img[rows(0, HALF), :] = low[:HALF]
    img[rows(256, HALF), :] = low[HALF:]

    pl.semaphore_wait(barrier, len(partners))

    ca, cb = {}, {}

    def sem_of(first, i, j):
        return r_first.at[first * 3 + i - 1] if j == 0 else r_second.at[first * 3 + j - 1]

    def ship_a(tx, ty, sx, where):
        ca[(tx, ty)] = send(img.at[rows(sx * HALF, HALF), :], img.at[rows((ty * 4 + tx) * HALF, HALF), :],
                            0, sem_of(0, tx, ty), where)

    def ship_b(tx, ty, sy, where):
        cb[(tx, ty)] = send(img.at[rows(256 + sy * HALF, HALF), :],
                            img.at[rows(256 + (tx * 4 + ty) * HALF, HALF), :],
                            0, sem_of(1, ty, tx), where)

    def pair(first, j):
        start = first * 256 + j * 64
        if j > 0:
            wait_all(img.at[rows(start, 64), :], r_second.at[first * 3 + j - 1])
        send(img.at[rows(start, 64), :], img.at[rows(512 + start, 64), :], 2, r_pair, at(dk=1))

    order = (1, 3, 2)
    for i in order:
        ship_a(4 - i, 0, 0, at(dx=i))
        ship_b(0, 4 - i, 0, at(dy=i))
    for i in order:
        ship_a(0, 4 - i, 0, at(dy=i))
        ship_b(4 - i, 0, 0, at(dx=i))

    loads[1].wait()
    loads[2].wait()
    projected = jnp.dot(text_ref[...], head[...], preferred_element_type=F32)
    text_len = jnp.sqrt(jnp.sum(projected * projected, axis=-1, keepdims=True) + EPSILON)
    text_dir = projected / text_len
    tdir[...] = text_dir
    txt[rows(0, ROWS), :] = text_dir.astype(BF16)

    cz = {}

    def ship_zc(sign, step, half, c):
        src_slot = ((8 - (step - 1)) % 8) if sign > 0 else step - 1
        dst_slot = (8 - step) if sign > 0 else step
        n = (((0 if sign > 0 else 4) + step - 1) * 2 + half) * 2 + c
        cz[(sign, step, half, c)] = send(
            txt.at[rows(TEXT_ROW[src_slot] + half * HALF, HALF), pl.ds(*CHUNKS[c])],
            txt.at[rows(TEXT_ROW[dst_slot] + half * HALF, HALF), pl.ds(*CHUNKS[c])],
            1, r_z.at[n], at(dz=sign))

    for half in range(2):
        for c in range(2):
            ship_zc(1, 1, half, c)
            ship_zc(-1, 1, half, c)

    def forward_image(i):
        ca[(i, 0)].wait_recv()
        for j in order:
            ship_a(i, 4 - j, i, at(dy=j))
        cb[(0, i)].wait_recv()
        for j in order:
            ship_b(4 - j, i, i, at(dx=j))

    column = lax.broadcasted_iota(jnp.int32, (1, COLS), 1)
    source = column
    for n in range(1, NZ):
        source = source + jnp.where(column >= n * SLICE, COLS - SLICE, 0)
    entry = lax.broadcasted_iota(jnp.int32, (D, COLS), 0)

    def select(q):
        chosen = jnp.where(entry == source + q * SLICE, 1.0, 0.0).astype(BF16)
        fsel_ref[q] = jnp.dot(text_ref[...], chosen, preferred_element_type=F32).astype(BF16)

    forward_image(3)
    forward_image(1)
    for step in (1, 2, 3):
        for half in range(2):
            for c in range(2):
                cz[(1, step, half, c)].wait_recv()
                if step < 3 or half == 0:
                    ship_zc(1, step + 1, half, c)
                cz[(-1, step, half, c)].wait_recv()
                if step < 3 or half == 1:
                    ship_zc(-1, step + 1, half, c)
        if step == 1:
            forward_image(2)
            pair(0, 0)
            pair(1, 0)
            pl.loop(0, 4)(select)
        if step == 2:
            pl.loop(4, 8)(select)
            for j in (1, 3):
                pair(0, j)
                pair(1, j)
        if step == 3:
            pair(0, 2)
            pair(1, 2)
    for c in range(2):
        cz[(1, 4, 0, c)].wait_recv()
        cz[(-1, 4, 1, c)].wait_recv()
    wait_all(img.at[rows(512, 512), :], r_pair)

    factor = jnp.exp(jnp.full((1, 1), scalar_ref[0], F32))
    offset = scalar_ref[1]

    def tile(i):
        part = rows(i * 128, 128)
        logits = factor * lax.dot_general(
            txt[part, :], img[...], (((1,), (1,)), ((), ())), preferred_element_type=F32) + offset
        prob = jax.nn.sigmoid(logits)
        if i == 0:
            row = lax.broadcasted_iota(jnp.int32, (128, IMAGES), 0)
            col = lax.broadcasted_iota(jnp.int32, (128, IMAGES), 1)
            want = jnp.where(row < HALF, row, row + 240)
            prob = prob - jnp.where((row < ROWS) & (col == want), 1.0, 0.0).astype(F32)
        weights = (factor * prob).astype(BF16)
        wt[part, :] = weights
        tp[part, :] = jnp.dot(weights, img[...], preferred_element_type=F32).astype(BF16)

    cr = {}

    def rz_slot(sign, dist, half):
        return ((0 if sign > 0 else 4) + dist - 1) * 2 + half

    def ship_rs(sign, dist, half, c):
        slot = dist if sign > 0 else (8 - dist)
        n = rz_slot(sign, dist, half)
        cols = pl.ds(*CHUNKS[c])
        cr[(sign, dist, half, c)] = send(
            tp.at[rows(TEXT_ROW[slot] + half * HALF, HALF), cols], rz.at[n, :, cols],
            1, r_rs1 if dist == 1 else r_rs.at[n * 2 + c], at(dz=sign))

    def take_rs(sign, dist, half):
        slot = (dist - 1) if sign > 0 else (9 - dist)
        part = rows(TEXT_ROW[slot] + half * HALF, HALF)
        for c in range(2):
            cols = pl.ds(*CHUNKS[c])
            cr[(sign, dist, half, c)].wait_recv()
            tp[part, cols] = (
                tp[part, cols].astype(F32) + rz[rz_slot(sign, dist, half), :, cols].astype(F32)
            ).astype(BF16)
            ship_rs(sign, dist - 1, half, c)

    def image_tile(i):
        part = rows(i * 256, 256)
        ip[part, :] = lax.dot_general(
            wt[:, part], txt[...], (((0,), (0,)), ((), ())), preferred_element_type=F32).astype(BF16)

    ci = {}

    def ship_ir(name, dist, src, dst, n, where):
        ci[(name, dist)] = send(src, dst, 4, r_ir.at[n], where)

    def give_image(first):
        image_tile(2 + first)
        return send(ip.at[rows(512 + first * 256, 256), :], ipd.at[rows(first * 256, 256), :],
                    3, r_ex.at[first], at(dk=1))

    def join_image(first, copy):
        copy.wait_recv()

        def add(j):
            part = rows(pl.multiple_of(first * 256 + j * ROWS, ROWS), ROWS)
            ip[part, :] = (ip[part, :].astype(F32) + ipd[part, :].astype(F32)).astype(BF16)

        pl.loop(0, 8)(add)

    tile(1)
    for c in range(2):
        ship_rs(1, 4, 0, c)
        ship_rs(-1, 4, 1, c)
        ship_rs(1, 3, 1, c)
        ship_rs(-1, 3, 0, c)
    tile(0)
    take_rs(1, 4, 0)
    take_rs(-1, 4, 1)
    take_rs(1, 3, 1)
    take_rs(-1, 3, 0)
    ex = [give_image(0), give_image(1)]
    fall[0] = fsel_ref[k * 4 + x]
    for dk in range(2):
        for dx in range(4):
            if dk == 0 and dx == 0:
                continue
            slot = ((4 - dx) % 4) + 4 * dk
            send(fsel_ref.at[((k + dk) % 2) * 4 + (x + dx) % 4], fall.at[slot], 6, r_f, at(dx=dx, dk=dk))
    image_tile(0)
    image_tile(1)
    take_rs(1, 3, 0)
    take_rs(-1, 3, 1)
    take_rs(1, 2, 1)
    take_rs(-1, 2, 0)
    join_image(0, ex[0])
    for i in order:
        ship_ir("ay", i, ip.at[rows(i * 64, 64), :], iay.at[i - 1], 0, at(dy=i))
    join_image(1, ex[1])
    for i in order:
        ship_ir("bx", i, ip.at[rows(256 + i * 64, 64), :], ibx.at[i - 1], 1, at(dx=i))

    def fold(base, recv, name):
        wait_all(recv, r_ir.at[0 if name == "ay" else 1])
        for j in range(4):
            part = rows(base + j * HALF, HALF)
            inner = rows(j * HALF, HALF)
            total = ip[part, :].astype(F32)
            for i in range(3):
                total = total + recv[i, inner, :].astype(F32)
            ip[part, :] = total.astype(BF16)

    take_rs(1, 2, 0)
    take_rs(-1, 2, 1)

    wait_all(rz.at[pl.ds(0, 4)], r_rs1)
    halves = []
    for half in range(2):
        total = tp[rows(half * HALF, HALF), :].astype(F32)
        total = total + rz[rz_slot(1, 1, half)].astype(F32) + rz[rz_slot(-1, 1, half)].astype(F32)
        halves.append(total)
    text_sum = jnp.concatenate(halves, axis=0)
    text_dir = tdir[...]
    proj_grad = (
        (text_sum - text_dir * jnp.sum(text_dir * text_sum, axis=-1, keepdims=True)) / text_len
    ).astype(BF16)
    pall[0] = proj_grad

    cp = {}
    for dx in order:
        slot = 4 - dx
        cp[slot] = send(pall.at[0], pall.at[slot], 5, r_p.at[slot - 1], at(dx=dx))
    send(pall.at[0], pall.at[4], 5, r_pk, at(dk=1))

    gt_ref[...] = lax.dot_general(
        proj_grad, head[...], (((1,), (1,)), ((), ())), preferred_element_type=F32).astype(BF16)

    outs = [
        pltpu.make_async_copy(src, dst, out_sem.at[n])
        for n, (src, dst) in enumerate(((gi_ref, gi_hbm), (gt_ref, gt_hbm), (gh_ref, gh_hbm)))
    ]
    outs[1].start()
    fold(0, iay, "ay")
    for i in order:
        ship_ir("ax", i, ip.at[rows(i * HALF, HALF), :], iax.at[i - 1], 2, at(dx=i))
    fold(256, ibx, "bx")
    for i in order:
        ship_ir("by", i, ip.at[rows(256 + i * HALF, HALF), :], iby.at[i - 1], 3, at(dy=i))

    for slot in (1, 3, 2):
        cp[slot].wait_recv()
        send(pall.at[slot], pall.at[4 + slot], 5, r_pk, at(dk=1))
    wait_all(pall.at[pl.ds(4, 4)], r_pk)
    wait_all(fall.at[pl.ds(1, 7)], r_f)

    hp[...] = lax.dot_general(
        fall[...].reshape(256, COLS), pall[...].reshape(256, D), (((0,), (0,)), ((), ())),
        preferred_element_type=F32)
    for s in range(NZ):
        part = hp[rows(s * SLICE, SLICE), :]
        hm[s] = part[:HALF].astype(BF16)
        hl[s] = part[HALF:].astype(BF16)
    for dz in (4, 3, 5, 2, 6, 1, 7):
        dest = (z + dz) % NZ
        send(hm.at[dest], rm.at[dz], 7, r_hm, at(dz=dz))
        send(hl.at[dest], rl.at[dz], 8, r_hl, at(dz=dz))

    wait_all(iax, r_ir.at[2])
    wait_all(iby, r_ir.at[3])
    total_a = ip[rows(0, HALF), :].astype(F32)
    total_b = ip[rows(256, HALF), :].astype(F32)
    for i in range(3):
        total_a = total_a + iax[i].astype(F32)
        total_b = total_b + iby[i].astype(F32)
    image_sum = jnp.concatenate([total_a, total_b], axis=0)
    wide = image_ref[...].astype(F32)
    image_len = jnp.sqrt(jnp.sum(wide * wide, axis=-1, keepdims=True) + EPSILON)
    image_dir = wide / image_len
    gi_ref[...] = (
        (image_sum - image_dir * jnp.sum(image_dir * image_sum, axis=-1, keepdims=True)) / image_len
    ).astype(BF16)

    outs[0].start()
    main = hm[z].astype(F32)
    left = hl[z].astype(F32)
    wait_all(rm.at[pl.ds(1, 7)], r_hm)
    wait_all(rl.at[pl.ds(1, 7)], r_hl)
    for dz in (1, 7, 2, 6, 3, 5, 4):
        main = main + rm[dz].astype(F32)
        left = left + rl[dz].astype(F32)
    sm[...] = main.astype(BF16)
    sl[...] = left.astype(BF16)

    y_lo = y % 2

    def final(target_y, target_k, slot):
        return (
            pltpu.make_async_remote_copy(
                src_ref=sm, dst_ref=qm.at[slot], send_sem=s_q.at[target_y // 2 * 2 + target_k],
                recv_sem=r_q.at[slot], device_id=device(x, target_y, z, target_k), device_id_type=MESH),
            pltpu.make_async_remote_copy(
                src_ref=sl, dst_ref=ql.at[slot], send_sem=s_q.at[4 + target_y // 2 * 2 + target_k],
                recv_sem=r_q.at[4 + slot], device_id=device(x, target_y, z, target_k), device_id_type=MESH),
        )

    for h in range(2):
        for tk in range(2):
            ty = k + 2 * h
            own = (ty == y) & (tk == k)

            @pl.when(jnp.logical_not(own))
            def _():
                for copy in final(ty, tk, y):
                    copy.start()

            @pl.when(own)
            def _():
                qm[y] = sm[...]
                ql[y] = sl[...]

    for sy in range(4):
        @pl.when(jnp.logical_not((sy == y) & (k == y_lo)))
        def _():
            for copy in final(y, k, sy):
                copy.wait_recv()

    main = qm[0].astype(F32)
    left = ql[0].astype(F32)
    for sy in range(1, 4):
        main = main + qm[sy].astype(F32)
        left = left + ql[sy].astype(F32)
    gh_ref[pl.ds(0, HALF), :] = main
    gh_ref[pl.ds(HALF, 2), :] = left
    outs[2].start()

    for n, ref in enumerate((
        img.at[rows(0, 480), :],
        img.at[rows(0, 448), :],
        img.at[rows(0, 512), :],
        img.at[rows(0, 512), :],
        img.at[rows(0, 480), :],
        pall.at[pl.ds(0, 7)],
        fall.at[pl.ds(0, 7)],
        rm.at[pl.ds(0, 7)],
        rl.at[pl.ds(0, 7)],
    )):
        wait_all(ref, s_all.at[n])
    for h in range(2):
        for tk in range(2):
            ty = k + 2 * h

            @pl.when(jnp.logical_not((ty == y) & (tk == k)))
            def _():
                for copy in final(ty, tk, y):
                    copy.wait_send()
    for copy in outs:
        copy.wait()


def deliver(gi_in, gt_in, gh_in, gi_out, gt_out, gh_out, gi_ref, gt_ref, gh_ref, in_sem, out_sem):
    first = [
        pltpu.make_async_copy(src, dst, in_sem.at[n])
        for n, (src, dst) in enumerate(((gi_in, gi_ref), (gt_in, gt_ref), (gh_in, gh_ref)))
    ]
    second = [
        pltpu.make_async_copy(src, dst, out_sem.at[n])
        for n, (src, dst) in enumerate(((gi_ref, gi_out), (gt_ref, gt_out), (gh_ref, gh_out)))
    ]
    for copy in first:
        copy.start()
    for n in range(3):
        first[n].wait()
        second[n].start()
    for copy in second:
        copy.wait()


def local(image_embed, text_feature, text_head, log_scale, bias):
    hbm = pl.BlockSpec(memory_space=pltpu.HBM)
    dma = pltpu.SemaphoreType.DMA
    V = pltpu.VMEM
    shapes = (
        jax.ShapeDtypeStruct((ROWS, D), BF16),
        jax.ShapeDtypeStruct((ROWS, D), BF16),
        jax.ShapeDtypeStruct((SLICE, D), F32),
    )
    results = pl.pallas_call(
        kernel,
        out_shape=shapes,
        in_specs=[pl.BlockSpec(memory_space=pltpu.SMEM)] + [hbm] * 3,
        out_specs=(hbm, hbm, hbm),
        scratch_shapes=[
            V((ROWS, D), BF16),
            V((ROWS, D), BF16),
            V((SLICE, D), F32),
            V((ROWS, D), BF16),
            V((ROWS, D), BF16),
            V((8, ROWS, COLS), BF16),
            V((D, D), BF16),
            V((IMAGES, D), BF16),
            V((TEXTS, D), BF16),
            V((TEXTS, IMAGES), BF16),
            V((TEXTS, D), BF16),
            V((IMAGES, D), BF16),
            V((16, HALF, D), BF16),
            V((3, 64, D), BF16),
            V((3, HALF, D), BF16),
            V((3, 64, D), BF16),
            V((3, HALF, D), BF16),
            V((512, D), BF16),
            V((ROWS, D), F32),
            V((8, ROWS, D), BF16),
            V((8, ROWS, COLS), BF16),
            V((COLS, D), F32),
            V((NZ, HALF, D), BF16),
            V((NZ, 2, D), BF16),
            V((NZ, HALF, D), BF16),
            V((NZ, 2, D), BF16),
            V((HALF, D), BF16),
            V((2, D), BF16),
            V((4, HALF, D), BF16),
            V((4, 2, D), BF16),
            dma((3,)), dma((3,)),
            dma((6,)), dma((6,)), dma, dma((32,)), dma, dma((32,)), dma, dma((2,)), dma((4,)),
            dma((3,)), dma, dma, dma, dma((8,)), dma((8,)), dma((9,)),
        ],
        compiler_params=pltpu.CompilerParams(
            collective_id=0, has_side_effects=True, vmem_limit_bytes=66500000),
        name="contrastive",
    )(jnp.concatenate([log_scale, bias]), image_embed, text_feature, text_head)
    return pl.pallas_call(
        deliver,
        out_shape=shapes,
        in_specs=[hbm] * 3,
        out_specs=(hbm, hbm, hbm),
        scratch_shapes=[
            V((ROWS, D), BF16), V((ROWS, D), BF16), V((SLICE, D), F32), dma((3,)), dma((3,))],
        compiler_params=pltpu.CompilerParams(vmem_limit_bytes=66500000),
        name="deliver",
    )(*results)


def solution(mesh):
    both = P(("grp", "blk"), None)
    return jax.shard_map(
        local,
        mesh=mesh,
        in_specs=(both, both, P(), P(), P()),
        out_specs=(both, both, P("blk", None)),
        check_vma=False,
    )
```

```python
import jax
import jax.numpy as jnp
from jax import lax
from jax.experimental import pallas as pl
from jax.experimental.pallas import tpu as pltpu
from jax.sharding import PartitionSpec as P

MESH = pl.DeviceIdType.MESH
EPSILON = 1e-06
F32 = jnp.float32
BF16 = jnp.bfloat16
D = 1152
ROWS = 32
HALF = 16
NX, NY, NZ, NK = 4, 4, 8, 2
COLS = D // NZ
SLICE = 18


def place():
    grp = lax.axis_index("grp")
    blk = lax.axis_index("blk")
    return blk % 4, (grp // 2) * 2 + (blk // 4) % 2, blk // 8, grp % 2


def device(x, y, z, k):
    return ((y // 2) * 2 + k, z * 8 + (y % 2) * 4 + x)


TEXT_ROW = {s: n * ROWS for n, s in enumerate((0, 1, 7, 2, 6, 3, 5, 4))}
TEXTS = 256
IMAGES = 1024
CHUNKS = ((0, 640), (640, 512))


def rows(start, count):
    return pl.ds(start, count)


def kernel(
    scale_ref, bias_ref, image_hbm, text_hbm, head_hbm,
    gi_hbm, gt_hbm, gh_hbm,
    gi_ref, gt_ref, gh_ref, image_ref, text_ref, fsel_ref, head, img, txt, wt, tp, ip, rz, iay, iax, iby, ibx,
    ipd, tdir, pall, fall, hp, hm, hl, rm, rl, sm, sl, qm, ql,
    in_sem, out_sem, r_first, r_second, r_pair, r_z, r_f, r_rs, r_rs1, r_ex, r_ir,
    r_p, r_pk, r_hm, r_hl, s_q, r_q, s_all,
):
    x, y, z, k = place()

    def at(dx=0, dy=0, dz=0, dk=0):
        return device((x + dx) % NX, (y + dy) % NY, (z + dz) % NZ, (k + dk) % NK)

    def send(src, dst, group, rsem, where):
        copy = pltpu.make_async_remote_copy(
            src_ref=src, dst_ref=dst, send_sem=s_all.at[group], recv_sem=rsem,
            device_id=where, device_id_type=MESH,
        )
        copy.start()
        return copy

    def wait_all(ref, sem):
        pltpu.make_async_remote_copy(
            src_ref=ref, dst_ref=ref, send_sem=sem, recv_sem=sem,
            device_id=at(dk=1), device_id_type=MESH,
        ).wait_recv()

    loads = []
    for n, (src, dst) in enumerate((
        (image_hbm, image_ref), (head_hbm, head), (text_hbm, text_ref),
    )):
        loads.append(pltpu.make_async_copy(src, dst, in_sem.at[n]))
        loads[n].start()

    barrier = pltpu.get_barrier_semaphore()
    partners = (
        [dict(dx=i) for i in (1, 2, 3)]
        + [dict(dy=i) for i in (1, 2, 3)]
        + [dict(dz=i) for i in (1, 2, 6, 7)]
        + [dict(dk=1)]
    )
    for p in partners:
        pl.semaphore_signal(barrier, inc=1, device_id=at(**p), device_id_type=MESH)

    loads[0].wait()
    wide = image_ref[...].astype(F32)
    image_len = jnp.sqrt(jnp.sum(wide * wide, axis=-1, keepdims=True) + EPSILON)
    low = (wide / image_len).astype(BF16)
    img[rows(0, HALF), :] = low[:HALF]
    img[rows(256, HALF), :] = low[HALF:]

    pl.semaphore_wait(barrier, len(partners))

    ca, cb = {}, {}

    def sem_of(first, i, j):
        return r_first.at[first * 3 + i - 1] if j == 0 else r_second.at[first * 3 + j - 1]

    def ship_a(tx, ty, sx, where):
        ca[(tx, ty)] = send(img.at[rows(sx * HALF, HALF), :], img.at[rows((ty * 4 + tx) * HALF, HALF), :],
                            0, sem_of(0, tx, ty), where)

    def ship_b(tx, ty, sy, where):
        cb[(tx, ty)] = send(img.at[rows(256 + sy * HALF, HALF), :],
                            img.at[rows(256 + (tx * 4 + ty) * HALF, HALF), :],
                            0, sem_of(1, ty, tx), where)

    def pair(first, j):
        start = first * 256 + j * 64
        if j > 0:
            wait_all(img.at[rows(start, 64), :], r_second.at[first * 3 + j - 1])
        send(img.at[rows(start, 64), :], img.at[rows(512 + start, 64), :], 2, r_pair, at(dk=1))

    order = (1, 3, 2)
    for i in order:
        ship_a(4 - i, 0, 0, at(dx=i))
        ship_b(0, 4 - i, 0, at(dy=i))
    for i in order:
        ship_a(0, 4 - i, 0, at(dy=i))
        ship_b(4 - i, 0, 0, at(dx=i))

    loads[1].wait()
    loads[2].wait()
    projected = jnp.dot(text_ref[...], head[...], preferred_element_type=F32)
    text_len = jnp.sqrt(jnp.sum(projected * projected, axis=-1, keepdims=True) + EPSILON)
    text_dir = projected / text_len
    tdir[...] = text_dir
    txt[rows(0, ROWS), :] = text_dir.astype(BF16)

    cz = {}

    def ship_zc(sign, step, half, c):
        before = min(step - 1, 2)
        src_slot = ((8 - before) % 8) if sign > 0 else before
        dst_slot = (8 - step) if sign > 0 else step
        n = (((0 if sign > 0 else 4) + step - 1) * 2 + half) * 2 + c
        cz[(sign, step, half, c)] = send(
            txt.at[rows(TEXT_ROW[src_slot] + half * HALF, HALF), pl.ds(*CHUNKS[c])],
            txt.at[rows(TEXT_ROW[dst_slot] + half * HALF, HALF), pl.ds(*CHUNKS[c])],
            1, r_z.at[n], at(dz=sign * (step - before)))

    for half in range(2):
        for c in range(2):
            ship_zc(1, 1, half, c)
            ship_zc(-1, 1, half, c)

    def forward_image(i):
        ca[(i, 0)].wait_recv()
        for j in order:
            ship_a(i, 4 - j, i, at(dy=j))
        cb[(0, i)].wait_recv()
        for j in order:
            ship_b(4 - j, i, i, at(dx=j))

    column = lax.broadcasted_iota(jnp.int32, (1, COLS), 1)
    source = column
    for n in range(1, NZ):
        source = source + jnp.where(column >= n * SLICE, COLS - SLICE, 0)
    entry = lax.broadcasted_iota(jnp.int32, (D, COLS), 0)

    def select(q):
        chosen = jnp.where(entry == source + q * SLICE, 1.0, 0.0).astype(BF16)
        fsel_ref[q] = jnp.dot(text_ref[...], chosen, preferred_element_type=F32).astype(BF16)

    forward_image(3)
    forward_image(1)
    for step in (1, 2, 3):
        for half in range(2):
            for c in range(2):
                for sign in (1, -1):
                    cz[(sign, step, half, c)].wait_recv()
                    if step == 2 and half == (0 if sign > 0 else 1):
                        ship_zc(sign, 4, half, c)
                    if step < 3:
                        ship_zc(sign, step + 1, half, c)
        if step == 1:
            forward_image(2)
            pair(0, 0)
            pair(1, 0)
            pl.loop(0, 4)(select)
        if step == 2:
            pl.loop(4, 8)(select)
            for j in (1, 3):
                pair(0, j)
                pair(1, j)
        if step == 3:
            pair(0, 2)
            pair(1, 2)
    for c in range(2):
        cz[(1, 4, 0, c)].wait_recv()
        cz[(-1, 4, 1, c)].wait_recv()
    factor = jnp.exp(jnp.full((1, 1), scale_ref[0], F32))
    offset = bias_ref[0]

    def weigh(i, core):
        part = rows(i * 128, 128)
        logits = factor * lax.dot_general(
            txt[part, :], img[rows(core * 512, 512), :], (((1,), (1,)), ((), ())),
            preferred_element_type=F32) + offset
        prob = jax.nn.sigmoid(logits)
        if i == 0 and core == 0:
            row = lax.broadcasted_iota(jnp.int32, (128, 512), 0)
            col = lax.broadcasted_iota(jnp.int32, (128, 512), 1)
            want = jnp.where(row < HALF, row, row + 240)
            prob = prob - jnp.where((row < ROWS) & (col == want), 1.0, 0.0).astype(F32)
        wt[part, pl.ds(core * 512, 512)] = (factor * prob).astype(BF16)

    def tile(i):
        part = rows(i * 128, 128)
        tp[part, :] = jnp.dot(wt[part, :], img[...], preferred_element_type=F32).astype(BF16)

    cr = {}

    def rz_slot(sign, dist, half):
        return ((0 if sign > 0 else 4) + dist - 1) * 2 + half

    def ship_rs(sign, dist, half, c):
        slot = dist if sign > 0 else (8 - dist)
        n = rz_slot(sign, dist, half)
        cols = pl.ds(*CHUNKS[c])
        cr[(sign, dist, half, c)] = send(
            tp.at[rows(TEXT_ROW[slot] + half * HALF, HALF), cols], rz.at[n, :, cols],
            1, r_rs1 if dist == 1 else r_rs.at[n * 2 + c], at(dz=sign * (2 if dist == 4 else 1)))

    def take_rs(sign, dists, half, c):
        to = 2 if 4 in dists or 3 in dists else 1
        slot = to if sign > 0 else 8 - to
        part = rows(TEXT_ROW[slot] + half * HALF, HALF)
        cols = pl.ds(*CHUNKS[c])
        total = tp[part, cols].astype(F32)
        for dist in dists:
            cr[(sign, dist, half, c)].wait_recv()
            total = total + rz[rz_slot(sign, dist, half), :, cols].astype(F32)
        tp[part, cols] = total.astype(BF16)
        ship_rs(sign, to, half, c)

    def image_tile(i):
        part = rows(i * 256, 256)
        ip[part, :] = lax.dot_general(
            wt[:, part], txt[...], (((0,), (0,)), ((), ())), preferred_element_type=F32).astype(BF16)

    ci = {}

    def ship_ir(name, dist, src, dst, n, where):
        ci[(name, dist)] = send(src, dst, 4, r_ir.at[n], where)

    def give_image(first):
        image_tile(2 + first)
        return send(ip.at[rows(512 + first * 256, 256), :], ipd.at[rows(first * 256, 256), :],
                    3, r_ex.at[first], at(dk=1))

    def join_image(first, copy):
        copy.wait_recv()

        def add(j):
            part = rows(pl.multiple_of(first * 256 + j * ROWS, ROWS), ROWS)
            ip[part, :] = (ip[part, :].astype(F32) + ipd[part, :].astype(F32)).astype(BF16)

        pl.loop(0, 8)(add)

    weigh(1, 0)
    wait_all(img.at[rows(512, 512), :], r_pair)
    weigh(1, 1)
    tile(1)
    for c in range(2):
        ship_rs(1, 4, 0, c)
        ship_rs(-1, 4, 1, c)
        for half in range(2):
            ship_rs(1, 3, half, c)
            ship_rs(-1, 3, half, c)
    weigh(0, 0)
    weigh(0, 1)
    tile(0)
    ex = [give_image(0), give_image(1)]
    image_tile(0)
    image_tile(1)
    join_image(0, ex[0])
    for i in order:
        ship_ir("ay", i, ip.at[rows(i * 64, 64), :], iay.at[i - 1], 0, at(dy=i))
    join_image(1, ex[1])
    for i in order:
        for j in range(4):
            ship_ir("by", i, ip.at[rows(256 + j * 64 + i * HALF, HALF), :],
                    iby.at[i - 1, rows(j * HALF, HALF), :], 1, at(dy=i))
    for c in range(2):
        take_rs(1, (4, 3), 0, c)
        take_rs(-1, (4, 3), 1, c)
        take_rs(1, (3,), 1, c)
        take_rs(-1, (3,), 0, c)
    for c in range(2):
        for half in range(2):
            take_rs(1, (2,), half, c)
            take_rs(-1, (2,), half, c)
    fall[0] = fsel_ref[k * 4 + x]
    for dk in range(2):
        for dx in range(4):
            if dk == 0 and dx == 0:
                continue
            slot = ((4 - dx) % 4) + 4 * dk
            send(fsel_ref.at[((k + dk) % 2) * 4 + (x + dx) % 4], fall.at[slot], 6, r_f, at(dx=dx, dk=dk))

    def fold(base, step, recv, sem):
        wait_all(recv, sem)
        for j in range(4):
            part = rows(base + j * step, HALF)
            total = ip[part, :].astype(F32)
            for i in range(3):
                total = total + recv[i, rows(j * HALF, HALF), :].astype(F32)
            ip[part, :] = total.astype(BF16)

    wait_all(rz.at[pl.ds(0, 4)], r_rs1)
    halves = []
    for half in range(2):
        total = tp[rows(half * HALF, HALF), :].astype(F32)
        total = total + rz[rz_slot(1, 1, half)].astype(F32) + rz[rz_slot(-1, 1, half)].astype(F32)
        halves.append(total)
    text_sum = jnp.concatenate(halves, axis=0)
    text_dir = tdir[...]
    proj_grad = (
        (text_sum - text_dir * jnp.sum(text_dir * text_sum, axis=-1, keepdims=True)) / text_len
    ).astype(BF16)
    pall[0] = proj_grad

    cp = {}
    for dx in order:
        slot = 4 - dx
        cp[slot] = send(pall.at[0], pall.at[slot], 5, r_p.at[slot - 1], at(dx=dx))
    send(pall.at[0], pall.at[4], 5, r_pk, at(dk=1))

    gt_ref[...] = lax.dot_general(
        proj_grad, head[...], (((1,), (1,)), ((), ())), preferred_element_type=F32).astype(BF16)

    outs = [
        pltpu.make_async_copy(src, dst, out_sem.at[n])
        for n, (src, dst) in enumerate(((gi_ref, gi_hbm), (gt_ref, gt_hbm), (gh_ref, gh_hbm)))
    ]
    outs[1].start()
    for slot in (1, 3, 2):
        cp[slot].wait_recv()
        send(pall.at[slot], pall.at[4 + slot], 5, r_pk, at(dk=1))
    wait_all(pall.at[pl.ds(4, 4)], r_pk)
    wait_all(fall.at[pl.ds(1, 7)], r_f)

    hp[...] = lax.dot_general(
        fall[...].reshape(256, COLS), pall[...].reshape(256, D), (((0,), (0,)), ((), ())),
        preferred_element_type=F32)
    for s in range(NZ):
        part = hp[rows(s * SLICE, SLICE), :]
        hm[s] = part[:HALF].astype(BF16)
        hl[s] = part[HALF:].astype(BF16)
    for dz in (4, 3, 5, 2, 6, 1, 7):
        dest = (z + dz) % NZ
        send(hm.at[dest], rm.at[dz], 7, r_hm, at(dz=dz))
        send(hl.at[dest], rl.at[dz], 8, r_hl, at(dz=dz))

    fold(0, HALF, iay, r_ir.at[0])
    fold(256, 64, iby, r_ir.at[1])
    for i in order:
        ship_ir("ax", i, ip.at[rows(i * HALF, HALF), :], iax.at[i - 1], 2, at(dx=i))
        ship_ir("bx", i, ip.at[rows(256 + i * 64, HALF), :], ibx.at[i - 1], 3, at(dx=i))
    wait_all(iax, r_ir.at[2])
    wait_all(ibx, r_ir.at[3])
    total_a = ip[rows(0, HALF), :].astype(F32)
    total_b = ip[rows(256, HALF), :].astype(F32)
    for i in range(3):
        total_a = total_a + iax[i].astype(F32)
        total_b = total_b + ibx[i].astype(F32)
    image_sum = jnp.concatenate([total_a, total_b], axis=0)
    wide = image_ref[...].astype(F32)
    image_len = jnp.sqrt(jnp.sum(wide * wide, axis=-1, keepdims=True) + EPSILON)
    image_dir = wide / image_len
    gi_ref[...] = (
        (image_sum - image_dir * jnp.sum(image_dir * image_sum, axis=-1, keepdims=True)) / image_len
    ).astype(BF16)

    outs[0].start()
    main = hm[z].astype(F32)
    left = hl[z].astype(F32)
    wait_all(rm.at[pl.ds(1, 7)], r_hm)
    wait_all(rl.at[pl.ds(1, 7)], r_hl)
    for dz in (1, 7, 2, 6, 3, 5, 4):
        main = main + rm[dz].astype(F32)
        left = left + rl[dz].astype(F32)
    sm[...] = main.astype(BF16)
    sl[...] = left.astype(BF16)

    y_lo = y % 2

    def final(target_y, target_k, slot):
        return (
            pltpu.make_async_remote_copy(
                src_ref=sm, dst_ref=qm.at[slot], send_sem=s_q.at[target_y // 2 * 2 + target_k],
                recv_sem=r_q.at[slot], device_id=device(x, target_y, z, target_k), device_id_type=MESH),
            pltpu.make_async_remote_copy(
                src_ref=sl, dst_ref=ql.at[slot], send_sem=s_q.at[4 + target_y // 2 * 2 + target_k],
                recv_sem=r_q.at[4 + slot], device_id=device(x, target_y, z, target_k), device_id_type=MESH),
        )

    for h in range(2):
        for tk in range(2):
            ty = k + 2 * h
            own = (ty == y) & (tk == k)

            @pl.when(jnp.logical_not(own))
            def _():
                for copy in final(ty, tk, y):
                    copy.start()

            @pl.when(own)
            def _():
                qm[y] = sm[...]
                ql[y] = sl[...]

    for sy in range(4):
        @pl.when(jnp.logical_not((sy == y) & (k == y_lo)))
        def _():
            for copy in final(y, k, sy):
                copy.wait_recv()

    main = qm[0].astype(F32)
    left = ql[0].astype(F32)
    for sy in range(1, 4):
        main = main + qm[sy].astype(F32)
        left = left + ql[sy].astype(F32)
    gh_ref[pl.ds(0, HALF), :] = main
    gh_ref[pl.ds(HALF, 2), :] = left
    outs[2].start()

    for n, ref in enumerate((
        img.at[rows(0, 480), :],
        img.at[rows(0, 448), :],
        img.at[rows(0, 512), :],
        img.at[rows(0, 512), :],
        img.at[rows(0, 480), :],
        pall.at[pl.ds(0, 7)],
        fall.at[pl.ds(0, 7)],
        rm.at[pl.ds(0, 7)],
        rl.at[pl.ds(0, 7)],
    )):
        wait_all(ref, s_all.at[n])
    for h in range(2):
        for tk in range(2):
            ty = k + 2 * h

            @pl.when(jnp.logical_not((ty == y) & (tk == k)))
            def _():
                for copy in final(ty, tk, y):
                    copy.wait_send()
    for copy in outs:
        copy.wait()


def deliver(gi_in, gt_in, gh_in, gi_out, gt_out, gh_out, gi_ref, gt_ref, gh_ref, in_sem, out_sem):
    first = [
        pltpu.make_async_copy(src, dst, in_sem.at[n])
        for n, (src, dst) in enumerate(((gi_in, gi_ref), (gt_in, gt_ref), (gh_in, gh_ref)))
    ]
    second = [
        pltpu.make_async_copy(src, dst, out_sem.at[n])
        for n, (src, dst) in enumerate(((gi_ref, gi_out), (gt_ref, gt_out), (gh_ref, gh_out)))
    ]
    for copy in first:
        copy.start()
    for n in range(3):
        first[n].wait()
        second[n].start()
    for copy in second:
        copy.wait()


def local(image_embed, text_feature, text_head, log_scale, bias):
    hbm = pl.BlockSpec(memory_space=pltpu.HBM)
    dma = pltpu.SemaphoreType.DMA
    V = pltpu.VMEM
    shapes = (
        jax.ShapeDtypeStruct((ROWS, D), BF16),
        jax.ShapeDtypeStruct((ROWS, D), BF16),
        jax.ShapeDtypeStruct((SLICE, D), F32),
    )
    results = pl.pallas_call(
        kernel,
        out_shape=shapes,
        in_specs=[pl.BlockSpec(memory_space=pltpu.SMEM)] * 2 + [hbm] * 3,
        out_specs=(hbm, hbm, hbm),
        scratch_shapes=[
            V((ROWS, D), BF16),
            V((ROWS, D), BF16),
            V((SLICE, D), F32),
            V((ROWS, D), BF16),
            V((ROWS, D), BF16),
            V((8, ROWS, COLS), BF16),
            V((D, D), BF16),
            V((IMAGES, D), BF16),
            V((TEXTS, D), BF16),
            V((TEXTS, IMAGES), BF16),
            V((TEXTS, D), BF16),
            V((IMAGES, D), BF16),
            V((16, HALF, D), BF16),
            V((3, 64, D), BF16),
            V((3, HALF, D), BF16),
            V((3, 64, D), BF16),
            V((3, HALF, D), BF16),
            V((512, D), BF16),
            V((ROWS, D), F32),
            V((8, ROWS, D), BF16),
            V((8, ROWS, COLS), BF16),
            V((COLS, D), F32),
            V((NZ, HALF, D), BF16),
            V((NZ, 2, D), BF16),
            V((NZ, HALF, D), BF16),
            V((NZ, 2, D), BF16),
            V((HALF, D), BF16),
            V((2, D), BF16),
            V((4, HALF, D), BF16),
            V((4, 2, D), BF16),
            dma((3,)), dma((3,)),
            dma((6,)), dma((6,)), dma, dma((32,)), dma, dma((32,)), dma, dma((2,)), dma((4,)),
            dma((3,)), dma, dma, dma, dma((8,)), dma((8,)), dma((9,)),
        ],
        compiler_params=pltpu.CompilerParams(
            collective_id=0, has_side_effects=True, vmem_limit_bytes=66500000),
        name="contrastive",
    )(log_scale, bias, image_embed, text_feature, text_head)
    return pl.pallas_call(
        deliver,
        out_shape=shapes,
        in_specs=[hbm] * 3,
        out_specs=(hbm, hbm, hbm),
        scratch_shapes=[
            V((ROWS, D), BF16), V((ROWS, D), BF16), V((SLICE, D), F32), dma((3,)), dma((3,))],
        compiler_params=pltpu.CompilerParams(vmem_limit_bytes=66500000),
        name="deliver",
    )(*results)


def solution(mesh):
    both = P(("grp", "blk"), None)
    return jax.shard_map(
        local,
        mesh=mesh,
        in_specs=(both, both, P(), P(), P()),
        out_specs=(both, both, P("blk", None)),
        check_vma=False,
    )
```

```python
import jax
import jax.numpy as jnp
from jax import lax
from jax.experimental import pallas as pl
from jax.experimental.pallas import tpu as pltpu
from jax.sharding import PartitionSpec as P

MESH = pl.DeviceIdType.MESH
EPSILON = 1e-06
F32 = jnp.float32
BF16 = jnp.bfloat16
D = 1152
ROWS = 32
HALF = 16
NX, NY, NZ, NK = 4, 4, 8, 2
COLS = D // NZ
SLICE = 18


def place():
    grp = lax.axis_index("grp")
    blk = lax.axis_index("blk")
    return blk % 4, (grp // 2) * 2 + (blk // 4) % 2, blk // 8, grp % 2


def device(x, y, z, k):
    return ((y // 2) * 2 + k, z * 8 + (y % 2) * 4 + x)


TEXT_ROW = {s: n * ROWS for n, s in enumerate((0, 1, 7, 2, 6, 3, 5, 4))}
TEXTS = 256
IMAGES = 1024
CHUNKS = ((0, 640), (640, 512))


def rows(start, count):
    return pl.ds(start, count)


def kernel(
    scale_ref, bias_ref, image_hbm, text_hbm, head_hbm,
    gi_ref, gt_ref, gh_ref, image_ref, text_ref, fsel_ref, head, img, txt, wt, tp, ip, rz, iay, iax, iby, ibx,
    ipd, tdir, pall, fall, hp, hm, hl, rm, rl, sm, sl, qm, ql,
    in_sem, r_first, r_second, r_pair, r_z, r_f, r_rs, r_rs1, r_ex, r_ir,
    r_p, r_pk, r_hm, r_hl, s_q, r_q, s_all,
):
    x, y, z, k = place()

    def at(dx=0, dy=0, dz=0, dk=0):
        return device((x + dx) % NX, (y + dy) % NY, (z + dz) % NZ, (k + dk) % NK)

    def send(src, dst, group, rsem, where):
        copy = pltpu.make_async_remote_copy(
            src_ref=src, dst_ref=dst, send_sem=s_all.at[group], recv_sem=rsem,
            device_id=where, device_id_type=MESH,
        )
        copy.start()
        return copy

    def wait_all(ref, sem):
        pltpu.make_async_remote_copy(
            src_ref=ref, dst_ref=ref, send_sem=sem, recv_sem=sem,
            device_id=at(dk=1), device_id_type=MESH,
        ).wait_recv()

    loads = []
    for n, (src, dst) in enumerate((
        (image_hbm, image_ref), (head_hbm, head), (text_hbm, text_ref),
    )):
        loads.append(pltpu.make_async_copy(src, dst, in_sem.at[n]))
        loads[n].start()

    barrier = pltpu.get_barrier_semaphore()
    partners = (
        [dict(dx=i) for i in (1, 2, 3)]
        + [dict(dy=i) for i in (1, 2, 3)]
        + [dict(dz=i) for i in (1, 2, 6, 7)]
        + [dict(dk=1)]
    )
    for p in partners:
        pl.semaphore_signal(barrier, inc=1, device_id=at(**p), device_id_type=MESH)

    loads[0].wait()
    wide = image_ref[...].astype(F32)
    image_len = jnp.sqrt(jnp.sum(wide * wide, axis=-1, keepdims=True) + EPSILON)
    low = (wide / image_len).astype(BF16)
    img[rows(0, HALF), :] = low[:HALF]
    img[rows(256, HALF), :] = low[HALF:]

    pl.semaphore_wait(barrier, len(partners))

    ca, cb = {}, {}

    def sem_of(first, i, j):
        return r_first.at[first * 3 + i - 1] if j == 0 else r_second.at[first * 3 + j - 1]

    def ship_a(tx, ty, sx, where):
        ca[(tx, ty)] = send(img.at[rows(sx * HALF, HALF), :], img.at[rows((ty * 4 + tx) * HALF, HALF), :],
                            0, sem_of(0, tx, ty), where)

    def ship_b(tx, ty, sy, where):
        cb[(tx, ty)] = send(img.at[rows(256 + sy * HALF, HALF), :],
                            img.at[rows(256 + (tx * 4 + ty) * HALF, HALF), :],
                            0, sem_of(1, ty, tx), where)

    def pair(first, j):
        start = first * 256 + j * 64
        if j > 0:
            wait_all(img.at[rows(start, 64), :], r_second.at[first * 3 + j - 1])
        send(img.at[rows(start, 64), :], img.at[rows(512 + start, 64), :], 2, r_pair, at(dk=1))

    order = (1, 3, 2)
    for i in order:
        ship_a(4 - i, 0, 0, at(dx=i))
        ship_b(0, 4 - i, 0, at(dy=i))
    for i in order:
        ship_a(0, 4 - i, 0, at(dy=i))
        ship_b(4 - i, 0, 0, at(dx=i))

    loads[1].wait()
    loads[2].wait()
    projected = jnp.dot(text_ref[...], head[...], preferred_element_type=F32)
    text_len = jnp.sqrt(jnp.sum(projected * projected, axis=-1, keepdims=True) + EPSILON)
    text_dir = projected / text_len
    tdir[...] = text_dir
    txt[rows(0, ROWS), :] = text_dir.astype(BF16)

    cz = {}

    def ship_zc(sign, step, half, c):
        before = min(step - 1, 2)
        src_slot = ((8 - before) % 8) if sign > 0 else before
        dst_slot = (8 - step) if sign > 0 else step
        n = 16 if step > 2 else (((0 if sign > 0 else 2) + step - 1) * 2 + half) * 2 + c
        cz[(sign, step, half, c)] = send(
            txt.at[rows(TEXT_ROW[src_slot] + half * HALF, HALF), pl.ds(*CHUNKS[c])],
            txt.at[rows(TEXT_ROW[dst_slot] + half * HALF, HALF), pl.ds(*CHUNKS[c])],
            1, r_z.at[n], at(dz=sign * (step - before)))

    for half in range(2):
        for c in range(2):
            ship_zc(1, 1, half, c)
            ship_zc(-1, 1, half, c)

    def forward_image(i):
        ca[(i, 0)].wait_recv()
        for j in order:
            ship_a(i, 4 - j, i, at(dy=j))
        cb[(0, i)].wait_recv()
        for j in order:
            ship_b(4 - j, i, i, at(dx=j))

    column = lax.broadcasted_iota(jnp.int32, (1, COLS), 1)
    source = column
    for n in range(1, NZ):
        source = source + jnp.where(column >= n * SLICE, COLS - SLICE, 0)
    entry = lax.broadcasted_iota(jnp.int32, (D, COLS), 0)

    def select(q):
        chosen = jnp.where(entry == source + q * SLICE, 1.0, 0.0).astype(BF16)
        fsel_ref[q] = jnp.dot(text_ref[...], chosen, preferred_element_type=F32).astype(BF16)

    forward_image(3)
    forward_image(1)
    for step in (1, 2):
        for half in range(2):
            for c in range(2):
                for sign in (1, -1):
                    cz[(sign, step, half, c)].wait_recv()
                    if step == 2 and half == (0 if sign > 0 else 1):
                        ship_zc(sign, 4, half, c)
                    ship_zc(sign, step + 1, half, c)
        if step == 1:
            forward_image(2)
            pair(0, 0)
            pair(1, 0)
            pl.loop(0, 4)(select)
    pl.loop(4, 8)(select)
    for j in (1, 3, 2):
        pair(0, j)
        pair(1, j)
    wait_all(txt.at[rows(0, 96), :], r_z.at[16])

    factor = jnp.exp(jnp.full((1, 1), scale_ref[0], F32))
    offset = bias_ref[0]

    def weigh(i, core):
        part = rows(i * 128, 128)
        logits = factor * lax.dot_general(
            txt[part, :], img[rows(core * 512, 512), :], (((1,), (1,)), ((), ())),
            preferred_element_type=F32) + offset
        prob = jax.nn.sigmoid(logits)
        if i == 0 and core == 0:
            row = lax.broadcasted_iota(jnp.int32, (128, 512), 0)
            col = lax.broadcasted_iota(jnp.int32, (128, 512), 1)
            want = jnp.where(row < HALF, row, row + 240)
            prob = prob - jnp.where((row < ROWS) & (col == want), 1.0, 0.0).astype(F32)
        wt[part, pl.ds(core * 512, 512)] = (factor * prob).astype(BF16)

    def tile(i):
        part = rows(i * 128, 128)
        tp[part, :] = jnp.dot(wt[part, :], img[...], preferred_element_type=F32).astype(BF16)

    cr = {}

    def rz_slot(sign, dist, half):
        return ((0 if sign > 0 else 4) + dist - 1) * 2 + half

    def ship_rs(sign, dist, half, c):
        slot = dist if sign > 0 else (8 - dist)
        n = rz_slot(sign, dist, half)
        m = ((0 if sign > 0 else 2) + half) * 2 + c + 4 + 8 * (3 - dist)
        if dist == 4:
            m = (0 if sign > 0 else 2) + c
        cols = pl.ds(*CHUNKS[c])
        cr[(sign, dist, half, c)] = send(
            tp.at[rows(TEXT_ROW[slot] + half * HALF, HALF), cols], rz.at[n, :, cols],
            1, r_rs1 if dist == 1 else r_rs.at[m], at(dz=sign * (2 if dist == 4 else 1)))

    def take_rs(sign, dists, half, c):
        to = 2 if 4 in dists or 3 in dists else 1
        slot = to if sign > 0 else 8 - to
        part = rows(TEXT_ROW[slot] + half * HALF, HALF)
        cols = pl.ds(*CHUNKS[c])
        total = tp[part, cols].astype(F32)
        for dist in dists:
            cr[(sign, dist, half, c)].wait_recv()
            total = total + rz[rz_slot(sign, dist, half), :, cols].astype(F32)
        tp[part, cols] = total.astype(BF16)
        ship_rs(sign, to, half, c)

    def image_tile(i):
        part = rows(i * 256, 256)
        ip[part, :] = lax.dot_general(
            wt[:, part], txt[...], (((0,), (0,)), ((), ())), preferred_element_type=F32).astype(BF16)

    ci = {}

    def ship_ir(name, dist, src, dst, n, where):
        ci[(name, dist)] = send(src, dst, 4, r_ir.at[n], where)

    def give_image(first):
        image_tile(2 + first)
        return send(ip.at[rows(512 + first * 256, 256), :], ipd.at[rows(first * 256, 256), :],
                    3, r_ex.at[first], at(dk=1))

    def join_image(first, copy):
        copy.wait_recv()

        def add(j):
            part = rows(pl.multiple_of(first * 256 + j * ROWS, ROWS), ROWS)
            ip[part, :] = (ip[part, :].astype(F32) + ipd[part, :].astype(F32)).astype(BF16)

        pl.loop(0, 8)(add)

    weigh(1, 0)
    weigh(0, 0)
    wait_all(img.at[rows(512, 512), :], r_pair)
    weigh(1, 1)
    tile(1)
    for c in range(2):
        ship_rs(1, 4, 0, c)
        ship_rs(-1, 4, 1, c)
        for half in range(2):
            ship_rs(1, 3, half, c)
            ship_rs(-1, 3, half, c)
    weigh(0, 1)
    tile(0)
    ex = [give_image(0), give_image(1)]
    image_tile(0)
    image_tile(1)
    join_image(0, ex[0])
    for i in order:
        ship_ir("ay", i, ip.at[rows(i * 64, 64), :], iay.at[i - 1], 0, at(dy=i))
    join_image(1, ex[1])
    for i in order:
        for j in range(4):
            ship_ir("by", i, ip.at[rows(256 + j * 64 + i * HALF, HALF), :],
                    iby.at[i - 1, rows(j * HALF, HALF), :], 1, at(dy=i))
    for c in range(2):
        take_rs(1, (4, 3), 0, c)
        take_rs(-1, (4, 3), 1, c)
        take_rs(1, (3,), 1, c)
        take_rs(-1, (3,), 0, c)
    for c in range(2):
        for half in range(2):
            take_rs(1, (2,), half, c)
            take_rs(-1, (2,), half, c)
    fall[0] = fsel_ref[k * 4 + x]
    for dk in range(2):
        for dx in range(4):
            if dk == 0 and dx == 0:
                continue
            slot = ((4 - dx) % 4) + 4 * dk
            send(fsel_ref.at[((k + dk) % 2) * 4 + (x + dx) % 4], fall.at[slot], 6, r_f, at(dx=dx, dk=dk))

    def fold(base, step, recv, sem):
        wait_all(recv, sem)
        for j in range(4):
            part = rows(base + j * step, HALF)
            total = ip[part, :].astype(F32)
            for i in range(3):
                total = total + recv[i, rows(j * HALF, HALF), :].astype(F32)
            ip[part, :] = total.astype(BF16)

    wait_all(rz.at[pl.ds(0, 4)], r_rs1)
    halves = []
    for half in range(2):
        total = tp[rows(half * HALF, HALF), :].astype(F32)
        total = total + rz[rz_slot(1, 1, half)].astype(F32) + rz[rz_slot(-1, 1, half)].astype(F32)
        halves.append(total)
    text_sum = jnp.concatenate(halves, axis=0)
    text_dir = tdir[...]
    proj_grad = (
        (text_sum - text_dir * jnp.sum(text_dir * text_sum, axis=-1, keepdims=True)) / text_len
    ).astype(BF16)
    pall[0] = proj_grad

    cp = {}
    for dx in order:
        slot = 4 - dx
        cp[slot] = send(pall.at[0], pall.at[slot], 5, r_p.at[slot - 1], at(dx=dx))
    send(pall.at[0], pall.at[4], 5, r_pk, at(dk=1))

    gt_ref[...] = lax.dot_general(
        proj_grad, head[...], (((1,), (1,)), ((), ())), preferred_element_type=F32).astype(BF16)

    for slot in (1, 3, 2):
        cp[slot].wait_recv()
        send(pall.at[slot], pall.at[4 + slot], 5, r_pk, at(dk=1))
    wait_all(pall.at[pl.ds(4, 4)], r_pk)
    wait_all(fall.at[pl.ds(1, 7)], r_f)

    hp[...] = lax.dot_general(
        fall[...].reshape(256, COLS), pall[...].reshape(256, D), (((0,), (0,)), ((), ())),
        preferred_element_type=F32)
    for s in range(NZ):
        part = hp[rows(s * SLICE, SLICE), :]
        hm[s] = part[:HALF].astype(BF16)
        hl[s] = part[HALF:].astype(BF16)
    far = (4, 3, 5, 2, 6, 1, 7)
    for c in range(2):
        cols = pl.ds(*CHUNKS[c])
        for dz in far:
            dest = (z + dz) % NZ
            send(hm.at[dest, :, cols], rm.at[dz, :, cols], 7, r_hm.at[c], at(dz=dz))
            if c == 0:
                send(hl.at[dest], rl.at[dz], 8, r_hl, at(dz=dz))

    fold(0, HALF, iay, r_ir.at[0])
    fold(256, 64, iby, r_ir.at[1])
    for i in order:
        ship_ir("ax", i, ip.at[rows(i * HALF, HALF), :], iax.at[i - 1], 2, at(dx=i))
        ship_ir("bx", i, ip.at[rows(256 + i * 64, HALF), :], ibx.at[i - 1], 3, at(dx=i))
    wait_all(iax, r_ir.at[2])
    wait_all(ibx, r_ir.at[3])
    total_a = ip[rows(0, HALF), :].astype(F32)
    total_b = ip[rows(256, HALF), :].astype(F32)
    for i in range(3):
        total_a = total_a + iax[i].astype(F32)
        total_b = total_b + ibx[i].astype(F32)
    image_sum = jnp.concatenate([total_a, total_b], axis=0)
    wide = image_ref[...].astype(F32)
    image_len = jnp.sqrt(jnp.sum(wide * wide, axis=-1, keepdims=True) + EPSILON)
    image_dir = wide / image_len
    gi_ref[...] = (
        (image_sum - image_dir * jnp.sum(image_dir * image_sum, axis=-1, keepdims=True)) / image_len
    ).astype(BF16)

    y_lo = y % 2

    def piece(p, slot):
        if p == 2:
            return sl, ql.at[slot]
        return sm.at[:, pl.ds(*CHUNKS[p])], qm.at[slot, :, pl.ds(*CHUNKS[p])]

    def final(p, target_y, target_k, slot):
        src, dst = piece(p, slot)
        return pltpu.make_async_remote_copy(
            src_ref=src, dst_ref=dst, send_sem=s_q.at[p * 4 + target_y // 2 * 2 + target_k],
            recv_sem=r_q.at[p * 4 + slot], device_id=device(x, target_y, z, target_k), device_id_type=MESH)

    def scatter(pieces):
        for h in range(2):
            for tk in range(2):
                ty = k + 2 * h
                own = (ty == y) & (tk == k)

                @pl.when(jnp.logical_not(own))
                def _():
                    for p in pieces:
                        final(p, ty, tk, y).start()

                @pl.when(own)
                def _():
                    for p in pieces:
                        src, dst = piece(p, y)
                        dst[...] = src[...]

    def collect(pieces):
        for sy in range(4):
            @pl.when(jnp.logical_not((sy == y) & (k == y_lo)))
            def _():
                for p in pieces:
                    final(p, y, k, sy).wait_recv()

    def sum_z(own, recv):
        total = own.astype(F32)
        for dz in far:
            total = total + recv(dz).astype(F32)
        return total.astype(BF16)

    def sum_y(part):
        total = part(0).astype(F32)
        for sy in range(1, 4):
            total = total + part(sy).astype(F32)
        return total

    for c in range(2):
        cols = pl.ds(*CHUNKS[c])
        wait_all(rm.at[pl.ds(1, 7), :, cols], r_hm.at[c])
        sm[:, cols] = sum_z(hm[z, :, cols], lambda dz: rm[dz, :, cols])
        if c == 0:
            wait_all(rl.at[pl.ds(1, 7)], r_hl)
            sl[...] = sum_z(hl[z], lambda dz: rl[dz])
        scatter((0, 2) if c == 0 else (1,))
    for c in range(2):
        cols = pl.ds(*CHUNKS[c])
        collect((0, 2) if c == 0 else (1,))
        gh_ref[pl.ds(0, HALF), cols] = sum_y(lambda sy: qm[sy, :, cols])
        if c == 0:
            gh_ref[pl.ds(HALF, 2), :] = sum_y(lambda sy: ql[sy])

    for n, ref in enumerate((
        img.at[rows(0, 480), :],
        img.at[rows(0, 448), :],
        img.at[rows(0, 512), :],
        img.at[rows(0, 512), :],
        img.at[rows(0, 480), :],
        pall.at[pl.ds(0, 7)],
        fall.at[pl.ds(0, 7)],
        rm.at[pl.ds(0, 7)],
        rl.at[pl.ds(0, 7)],
    )):
        wait_all(ref, s_all.at[n])
    for h in range(2):
        for tk in range(2):
            ty = k + 2 * h

            @pl.when(jnp.logical_not((ty == y) & (tk == k)))
            def _():
                for p in range(3):
                    final(p, ty, tk, y).wait_send()


def deliver(gi_ref, gt_ref, gh_ref, gi_out, gt_out, gh_out, sem):
    copies = [
        pltpu.make_async_copy(src, dst, sem.at[n])
        for n, (src, dst) in enumerate(((gi_ref, gi_out), (gt_ref, gt_out), (gh_ref, gh_out)))
    ]
    for copy in copies:
        copy.start()
    for copy in copies:
        copy.wait()


def local(image_embed, text_feature, text_head, log_scale, bias):
    hbm = pl.BlockSpec(memory_space=pltpu.HBM)
    vmem = pl.BlockSpec(memory_space=pltpu.VMEM)
    dma = pltpu.SemaphoreType.DMA
    V = pltpu.VMEM
    shapes = (
        jax.ShapeDtypeStruct((ROWS, D), BF16),
        jax.ShapeDtypeStruct((ROWS, D), BF16),
        jax.ShapeDtypeStruct((SLICE, D), F32),
    )
    results = pl.pallas_call(
        kernel,
        out_shape=tuple(pltpu.VMEM(a.shape, a.dtype) for a in shapes),
        in_specs=[pl.BlockSpec(memory_space=pltpu.SMEM)] * 2 + [hbm] * 3,
        out_specs=(vmem, vmem, vmem),
        scratch_shapes=[
            V((ROWS, D), BF16),
            V((ROWS, D), BF16),
            V((8, ROWS, COLS), BF16),
            V((D, D), BF16),
            V((IMAGES, D), BF16),
            V((TEXTS, D), BF16),
            V((TEXTS, IMAGES), BF16),
            V((TEXTS, D), BF16),
            V((IMAGES, D), BF16),
            V((16, HALF, D), BF16),
            V((3, 64, D), BF16),
            V((3, HALF, D), BF16),
            V((3, 64, D), BF16),
            V((3, HALF, D), BF16),
            V((512, D), BF16),
            V((ROWS, D), F32),
            V((8, ROWS, D), BF16),
            V((8, ROWS, COLS), BF16),
            V((COLS, D), F32),
            V((NZ, HALF, D), BF16),
            V((NZ, 2, D), BF16),
            V((NZ, HALF, D), BF16),
            V((NZ, 2, D), BF16),
            V((HALF, D), BF16),
            V((2, D), BF16),
            V((4, HALF, D), BF16),
            V((4, 2, D), BF16),
            dma((3,)),
            dma((6,)), dma((6,)), dma, dma((17,)), dma, dma((20,)), dma, dma((2,)), dma((4,)),
            dma((3,)), dma, dma((2,)), dma, dma((12,)), dma((12,)), dma((9,)),
        ],
        compiler_params=pltpu.CompilerParams(
            collective_id=0, has_side_effects=True, vmem_limit_bytes=66500000),
        name="contrastive",
    )(log_scale, bias, image_embed, text_feature, text_head)
    return pl.pallas_call(
        deliver,
        out_shape=shapes,
        in_specs=[vmem] * 3,
        out_specs=(hbm, hbm, hbm),
        scratch_shapes=[dma((3,))],
        compiler_params=pltpu.CompilerParams(vmem_limit_bytes=2**20),
        name="deliver",
    )(*results)


def solution(mesh):
    both = P(("grp", "blk"), None)
    return jax.shard_map(
        local,
        mesh=mesh,
        in_specs=(both, both, P(), P(), P()),
        out_specs=(both, both, P("blk", None)),
        check_vma=False,
    )
```

```python
import jax
import jax.numpy as jnp
from jax import lax
from jax.experimental import pallas as pl
from jax.experimental.pallas import tpu as pltpu
from jax.sharding import PartitionSpec as P

MESH = pl.DeviceIdType.MESH
EPSILON = 1e-06
F32 = jnp.float32
BF16 = jnp.bfloat16
D = 1152
ROWS = 32
HALF = 16
NX, NY, NZ, NK = 4, 4, 8, 2
COLS = D // NZ
SLICE = 18


def place():
    grp = lax.axis_index("grp")
    blk = lax.axis_index("blk")
    return blk % 4, (grp // 2) * 2 + (blk // 4) % 2, blk // 8, grp % 2


def device(x, y, z, k):
    return ((y // 2) * 2 + k, z * 8 + (y % 2) * 4 + x)


TEXT_ROW = {s: n * ROWS for n, s in enumerate((0, 1, 7, 2, 6, 3, 5, 4))}
TEXTS = 256
IMAGES = 1024
CHUNKS = ((0, 640), (640, 512))
PIECES = ((0, 768), (768, 384))


def rows(start, count):
    return pl.ds(start, count)


def kernel(
    scale_ref, bias_ref, image_hbm, text_hbm, head_hbm,
    gi_ref, gt_ref, gh_ref, image_ref, text_ref, fsel_ref, head, img, txt, wt, tp, ip, rz, iay, iax, iby, ibx,
    ipd, tdir, pall, fall, hp, hm, hl, rm, rl, sm, sl, qm, ql,
    in_sem, r_first, r_second, r_pair, r_z, r_f, r_rs, r_rs1, r_ex, r_ir,
    r_p, r_pk, r_hm, r_hl, s_q, r_q, s_all,
):
    x, y, z, k = place()

    def at(dx=0, dy=0, dz=0, dk=0):
        return device((x + dx) % NX, (y + dy) % NY, (z + dz) % NZ, (k + dk) % NK)

    def send(src, dst, group, rsem, where):
        copy = pltpu.make_async_remote_copy(
            src_ref=src, dst_ref=dst, send_sem=s_all.at[group], recv_sem=rsem,
            device_id=where, device_id_type=MESH,
        )
        copy.start()
        return copy

    def wait_all(ref, sem):
        pltpu.make_async_remote_copy(
            src_ref=ref, dst_ref=ref, send_sem=sem, recv_sem=sem,
            device_id=at(dk=1), device_id_type=MESH,
        ).wait_recv()

    loads = []
    for n, (src, dst) in enumerate((
        (image_hbm, image_ref), (head_hbm, head), (text_hbm, text_ref),
    )):
        loads.append(pltpu.make_async_copy(src, dst, in_sem.at[n]))
        loads[n].start()

    barrier = pltpu.get_barrier_semaphore()
    partners = (
        [dict(dx=i) for i in (1, 2, 3)]
        + [dict(dy=i) for i in (1, 2, 3)]
        + [dict(dz=i) for i in (1, 2, 6, 7)]
        + [dict(dk=1)]
    )
    for p in partners:
        pl.semaphore_signal(barrier, inc=1, device_id=at(**p), device_id_type=MESH)

    loads[0].wait()
    wide = image_ref[...].astype(F32)
    image_len = jnp.sqrt(jnp.sum(wide * wide, axis=-1, keepdims=True) + EPSILON)
    low = (wide / image_len).astype(BF16)
    img[rows(0, HALF), :] = low[:HALF]
    img[rows(256, HALF), :] = low[HALF:]

    pl.semaphore_wait(barrier, len(partners))

    ca, cb = {}, {}

    def sem_of(first, i, j):
        return r_first.at[first * 3 + i - 1] if j == 0 else r_second.at[first * 3 + j - 1]

    def ship_a(tx, ty, sx, where):
        ca[(tx, ty)] = send(img.at[rows(sx * HALF, HALF), :], img.at[rows((ty * 4 + tx) * HALF, HALF), :],
                            0, sem_of(0, tx, ty), where)

    def ship_b(tx, ty, sy, where):
        cb[(tx, ty)] = send(img.at[rows(256 + sy * HALF, HALF), :],
                            img.at[rows(256 + (tx * 4 + ty) * HALF, HALF), :],
                            0, sem_of(1, ty, tx), where)

    def pair(first, j):
        start = first * 256 + j * 64
        if j > 0:
            wait_all(img.at[rows(start, 64), :], r_second.at[first * 3 + j - 1])
        send(img.at[rows(start, 64), :], img.at[rows(512 + start, 64), :], 2, r_pair, at(dk=1))

    order = (1, 3, 2)
    for i in order:
        ship_a(4 - i, 0, 0, at(dx=i))
        ship_b(0, 4 - i, 0, at(dy=i))
    for i in order:
        ship_a(0, 4 - i, 0, at(dy=i))
        ship_b(4 - i, 0, 0, at(dx=i))

    loads[1].wait()
    loads[2].wait()
    projected = jnp.dot(text_ref[...], head[...], preferred_element_type=F32)
    text_len = jnp.sqrt(jnp.sum(projected * projected, axis=-1, keepdims=True) + EPSILON)
    text_dir = projected / text_len
    tdir[...] = text_dir
    txt[rows(0, ROWS), :] = text_dir.astype(BF16)

    cz = {}

    def ship_zc(sign, step, half, c):
        before = min(step - 1, 2)
        src_slot = ((8 - before) % 8) if sign > 0 else before
        dst_slot = (8 - step) if sign > 0 else step
        n = 16 if step > 2 else (((0 if sign > 0 else 2) + step - 1) * 2 + half) * 2 + c
        cz[(sign, step, half, c)] = send(
            txt.at[rows(TEXT_ROW[src_slot] + half * HALF, HALF), pl.ds(*CHUNKS[c])],
            txt.at[rows(TEXT_ROW[dst_slot] + half * HALF, HALF), pl.ds(*CHUNKS[c])],
            1, r_z.at[n], at(dz=sign * (step - before)))

    for half in range(2):
        for c in range(2):
            ship_zc(1, 1, half, c)
            ship_zc(-1, 1, half, c)

    def forward_image(i):
        ca[(i, 0)].wait_recv()
        for j in order:
            ship_a(i, 4 - j, i, at(dy=j))
        cb[(0, i)].wait_recv()
        for j in order:
            ship_b(4 - j, i, i, at(dx=j))

    column = lax.broadcasted_iota(jnp.int32, (1, COLS), 1)
    source = column
    for n in range(1, NZ):
        source = source + jnp.where(column >= n * SLICE, COLS - SLICE, 0)
    entry = lax.broadcasted_iota(jnp.int32, (D, COLS), 0)

    def select(q):
        chosen = jnp.where(entry == source + q * SLICE, 1.0, 0.0).astype(BF16)
        fsel_ref[q] = jnp.dot(text_ref[...], chosen, preferred_element_type=F32).astype(BF16)

    forward_image(3)
    forward_image(1)
    for step in (1, 2):
        for half in range(2):
            for c in range(2):
                for sign in (1, -1):
                    cz[(sign, step, half, c)].wait_recv()
                    if step == 2 and half == (0 if sign > 0 else 1):
                        ship_zc(sign, 4, half, c)
                    ship_zc(sign, step + 1, half, c)
        if step == 1:
            forward_image(2)
            pair(0, 0)
            pair(1, 0)
            pl.loop(0, 4)(select)
    pl.loop(4, 8)(select)
    for j in (1, 3, 2):
        pair(0, j)
        pair(1, j)
    factor = jnp.exp(jnp.full((1, 1), scale_ref[0], F32))
    offset = bias_ref[0]

    def weigh(i, core):
        part = rows(i * 128, 128)
        logits = factor * lax.dot_general(
            txt[part, :], img[rows(core * 512, 512), :], (((1,), (1,)), ((), ())),
            preferred_element_type=F32) + offset
        prob = jax.nn.sigmoid(logits)
        if i == 0 and core == 0:
            row = lax.broadcasted_iota(jnp.int32, (128, 512), 0)
            col = lax.broadcasted_iota(jnp.int32, (128, 512), 1)
            want = jnp.where(row < HALF, row, row + 240)
            prob = prob - jnp.where((row < ROWS) & (col == want), 1.0, 0.0).astype(F32)
        wt[part, pl.ds(core * 512, 512)] = (factor * prob).astype(BF16)

    def tile(i):
        part = rows(i * 128, 128)
        tp[part, :] = jnp.dot(wt[part, :], img[...], preferred_element_type=F32).astype(BF16)

    cr = {}

    def rz_slot(sign, dist, half):
        return ((0 if sign > 0 else 4) + dist - 1) * 2 + half

    def ship_rs(sign, dist, half, c):
        slot = dist if sign > 0 else (8 - dist)
        n = rz_slot(sign, dist, half)
        m = ((0 if sign > 0 else 2) + half) * 2 + c + 4 + 8 * (3 - dist)
        if dist == 4:
            m = (0 if sign > 0 else 2) + c
        cols = pl.ds(*CHUNKS[c])
        cr[(sign, dist, half, c)] = send(
            tp.at[rows(TEXT_ROW[slot] + half * HALF, HALF), cols], rz.at[n, :, cols],
            1, r_rs1 if dist == 1 else r_rs.at[m], at(dz=sign * (2 if dist == 4 else 1)))

    def take_rs(sign, dists, half, c):
        to = 2 if 4 in dists or 3 in dists else 1
        slot = to if sign > 0 else 8 - to
        part = rows(TEXT_ROW[slot] + half * HALF, HALF)
        cols = pl.ds(*CHUNKS[c])
        total = tp[part, cols].astype(F32)
        for dist in dists:
            cr[(sign, dist, half, c)].wait_recv()
            total = total + rz[rz_slot(sign, dist, half), :, cols].astype(F32)
        tp[part, cols] = total.astype(BF16)
        ship_rs(sign, to, half, c)

    def image_tile(i):
        part = rows(i * 256, 256)
        ip[part, :] = lax.dot_general(
            wt[:, part], txt[...], (((0,), (0,)), ((), ())), preferred_element_type=F32).astype(BF16)

    ci = {}

    def ship_ir(name, dist, src, dst, n, where):
        ci[(name, dist)] = send(src, dst, 4, r_ir.at[n], where)

    def give_image(first):
        image_tile(2 + first)
        return send(ip.at[rows(512 + first * 256, 256), :], ipd.at[rows(first * 256, 256), :],
                    3, r_ex.at[first], at(dk=1))

    def join_image(first, copy):
        copy.wait_recv()

        def add(j):
            part = rows(pl.multiple_of(first * 256 + j * ROWS, ROWS), ROWS)
            ip[part, :] = (ip[part, :].astype(F32) + ipd[part, :].astype(F32)).astype(BF16)

        pl.loop(0, 8)(add)

    weigh(0, 0)
    wait_all(txt.at[rows(0, 96), :], r_z.at[16])
    weigh(1, 0)
    wait_all(img.at[rows(512, 512), :], r_pair)
    weigh(1, 1)
    tile(1)
    for c in range(2):
        ship_rs(1, 4, 0, c)
        ship_rs(-1, 4, 1, c)
        for half in range(2):
            ship_rs(1, 3, half, c)
            ship_rs(-1, 3, half, c)
    weigh(0, 1)
    tile(0)
    ex = [give_image(0), give_image(1)]
    image_tile(0)
    image_tile(1)
    for c in range(2):
        take_rs(1, (4, 3), 0, c)
        take_rs(-1, (4, 3), 1, c)
        take_rs(1, (3,), 1, c)
        take_rs(-1, (3,), 0, c)
    join_image(0, ex[0])
    for i in order:
        ship_ir("ay", i, ip.at[rows(i * 64, 64), :], iay.at[i - 1], 0, at(dy=i))
    join_image(1, ex[1])
    for i in order:
        for j in range(4):
            ship_ir("by", i, ip.at[rows(256 + j * 64 + i * HALF, HALF), :],
                    iby.at[i - 1, rows(j * HALF, HALF), :], 1, at(dy=i))
    for c in range(2):
        for half in range(2):
            take_rs(1, (2,), half, c)
            take_rs(-1, (2,), half, c)
    fall[0] = fsel_ref[k * 4 + x]
    for dk in range(2):
        for dx in range(4):
            if dk == 0 and dx == 0:
                continue
            slot = ((4 - dx) % 4) + 4 * dk
            send(fsel_ref.at[((k + dk) % 2) * 4 + (x + dx) % 4], fall.at[slot], 6, r_f, at(dx=dx, dk=dk))

    def fold(base, step, recv, sem):
        wait_all(recv, sem)
        for j in range(4):
            part = rows(base + j * step, HALF)
            total = ip[part, :].astype(F32)
            for i in range(3):
                total = total + recv[i, rows(j * HALF, HALF), :].astype(F32)
            ip[part, :] = total.astype(BF16)

    wait_all(rz.at[pl.ds(0, 4)], r_rs1)
    halves = []
    for half in range(2):
        total = tp[rows(half * HALF, HALF), :].astype(F32)
        total = total + rz[rz_slot(1, 1, half)].astype(F32) + rz[rz_slot(-1, 1, half)].astype(F32)
        halves.append(total)
    text_sum = jnp.concatenate(halves, axis=0)
    text_dir = tdir[...]
    proj_grad = (
        (text_sum - text_dir * jnp.sum(text_dir * text_sum, axis=-1, keepdims=True)) / text_len
    ).astype(BF16)
    pall[0] = proj_grad

    cp = {}
    for dx in order:
        slot = 4 - dx
        cp[slot] = send(pall.at[0], pall.at[slot], 5, r_p.at[slot - 1], at(dx=dx))
    send(pall.at[0], pall.at[4], 5, r_pk, at(dk=1))

    gt_ref[...] = lax.dot_general(
        proj_grad, head[...], (((1,), (1,)), ((), ())), preferred_element_type=F32).astype(BF16)

    for slot in (1, 3, 2):
        cp[slot].wait_recv()
        send(pall.at[slot], pall.at[4 + slot], 5, r_pk, at(dk=1))
    wait_all(pall.at[pl.ds(4, 4)], r_pk)
    wait_all(fall.at[pl.ds(1, 7)], r_f)

    hp[...] = lax.dot_general(
        fall[...].reshape(256, COLS), pall[...].reshape(256, D), (((0,), (0,)), ((), ())),
        preferred_element_type=F32)
    for s in range(NZ):
        part = hp[rows(s * SLICE, SLICE), :]
        hm[s] = part[:HALF].astype(BF16)
        hl[s] = part[HALF:].astype(BF16)
    far = (4, 3, 5, 2, 6, 1, 7)
    for c in range(2):
        cols = pl.ds(*PIECES[c])
        for dz in far:
            dest = (z + dz) % NZ
            send(hm.at[dest, :, cols], rm.at[dz, :, cols], 7, r_hm.at[c], at(dz=dz))
            if c == 0:
                send(hl.at[dest], rl.at[dz], 8, r_hl, at(dz=dz))

    fold(0, HALF, iay, r_ir.at[0])
    fold(256, 64, iby, r_ir.at[1])
    for i in order:
        ship_ir("ax", i, ip.at[rows(i * HALF, HALF), :], iax.at[i - 1], 2, at(dx=i))
        ship_ir("bx", i, ip.at[rows(256 + i * 64, HALF), :], ibx.at[i - 1], 3, at(dx=i))
    y_lo = y % 2

    def piece(p, slot):
        if p == 2:
            return sl, ql.at[slot]
        return sm.at[:, pl.ds(*PIECES[p])], qm.at[slot, :, pl.ds(*PIECES[p])]

    def final(p, target_y, target_k, slot):
        src, dst = piece(p, slot)
        return pltpu.make_async_remote_copy(
            src_ref=src, dst_ref=dst, send_sem=s_q.at[p * 4 + target_y // 2 * 2 + target_k],
            recv_sem=r_q.at[p * 4 + slot], device_id=device(x, target_y, z, target_k), device_id_type=MESH)

    def scatter(pieces):
        for h in range(2):
            for tk in range(2):
                ty = k + 2 * h
                own = (ty == y) & (tk == k)

                @pl.when(jnp.logical_not(own))
                def _():
                    for p in pieces:
                        final(p, ty, tk, y).start()

                @pl.when(own)
                def _():
                    for p in pieces:
                        src, dst = piece(p, y)
                        dst[...] = src[...]

    def collect(pieces):
        for sy in range(4):
            @pl.when(jnp.logical_not((sy == y) & (k == y_lo)))
            def _():
                for p in pieces:
                    final(p, y, k, sy).wait_recv()

    def sum_z(own, recv):
        total = own.astype(F32)
        for dz in far:
            total = total + recv(dz).astype(F32)
        return total.astype(BF16)

    def sum_y(part):
        total = part(0).astype(F32)
        for sy in range(1, 4):
            total = total + part(sy).astype(F32)
        return total

    def finish_image():
        wait_all(iax, r_ir.at[2])
        wait_all(ibx, r_ir.at[3])
        total_a = ip[rows(0, HALF), :].astype(F32)
        total_b = ip[rows(256, HALF), :].astype(F32)
        for i in range(3):
            total_a = total_a + iax[i].astype(F32)
            total_b = total_b + ibx[i].astype(F32)
        image_sum = jnp.concatenate([total_a, total_b], axis=0)
        wide = image_ref[...].astype(F32)
        image_len = jnp.sqrt(jnp.sum(wide * wide, axis=-1, keepdims=True) + EPSILON)
        image_dir = wide / image_len
        gi_ref[...] = (
            (image_sum - image_dir * jnp.sum(image_dir * image_sum, axis=-1, keepdims=True)) / image_len
        ).astype(BF16)

    for c in range(2):
        cols = pl.ds(*PIECES[c])
        wait_all(rm.at[pl.ds(1, 7), :, cols], r_hm.at[c])
        sm[:, cols] = sum_z(hm[z, :, cols], lambda dz: rm[dz, :, cols])
        if c == 0:
            wait_all(rl.at[pl.ds(1, 7)], r_hl)
            sl[...] = sum_z(hl[z], lambda dz: rl[dz])
        scatter((0, 2) if c == 0 else (1,))
        if c == 0:
            finish_image()
    for c in range(2):
        cols = pl.ds(*PIECES[c])
        collect((0, 2) if c == 0 else (1,))
        gh_ref[pl.ds(0, HALF), cols] = sum_y(lambda sy: qm[sy, :, cols])
        if c == 0:
            gh_ref[pl.ds(HALF, 2), :] = sum_y(lambda sy: ql[sy])

    for n, ref in enumerate((
        img.at[rows(0, 480), :],
        img.at[rows(0, 448), :],
        img.at[rows(0, 512), :],
        img.at[rows(0, 512), :],
        img.at[rows(0, 480), :],
        pall.at[pl.ds(0, 7)],
        fall.at[pl.ds(0, 7)],
        rm.at[pl.ds(0, 7)],
        rl.at[pl.ds(0, 7)],
    )):
        wait_all(ref, s_all.at[n])
    for h in range(2):
        for tk in range(2):
            ty = k + 2 * h

            @pl.when(jnp.logical_not((ty == y) & (tk == k)))
            def _():
                for p in range(3):
                    final(p, ty, tk, y).wait_send()


def deliver(gi_ref, gt_ref, gh_ref, gi_out, gt_out, gh_out, sem):
    copies = [
        pltpu.make_async_copy(src, dst, sem.at[n])
        for n, (src, dst) in enumerate(((gi_ref, gi_out), (gt_ref, gt_out), (gh_ref, gh_out)))
    ]
    for copy in copies:
        copy.start()
    for copy in copies:
        copy.wait()


def local(image_embed, text_feature, text_head, log_scale, bias):
    hbm = pl.BlockSpec(memory_space=pltpu.HBM)
    vmem = pl.BlockSpec(memory_space=pltpu.VMEM)
    dma = pltpu.SemaphoreType.DMA
    V = pltpu.VMEM
    shapes = (
        jax.ShapeDtypeStruct((ROWS, D), BF16),
        jax.ShapeDtypeStruct((ROWS, D), BF16),
        jax.ShapeDtypeStruct((SLICE, D), F32),
    )
    results = pl.pallas_call(
        kernel,
        out_shape=tuple(pltpu.VMEM(a.shape, a.dtype) for a in shapes),
        in_specs=[pl.BlockSpec(memory_space=pltpu.SMEM)] * 2 + [hbm] * 3,
        out_specs=(vmem, vmem, vmem),
        scratch_shapes=[
            V((ROWS, D), BF16),
            V((ROWS, D), BF16),
            V((8, ROWS, COLS), BF16),
            V((D, D), BF16),
            V((IMAGES, D), BF16),
            V((TEXTS, D), BF16),
            V((TEXTS, IMAGES), BF16),
            V((TEXTS, D), BF16),
            V((IMAGES, D), BF16),
            V((16, HALF, D), BF16),
            V((3, 64, D), BF16),
            V((3, HALF, D), BF16),
            V((3, 64, D), BF16),
            V((3, HALF, D), BF16),
            V((512, D), BF16),
            V((ROWS, D), F32),
            V((8, ROWS, D), BF16),
            V((8, ROWS, COLS), BF16),
            V((COLS, D), F32),
            V((NZ, HALF, D), BF16),
            V((NZ, 2, D), BF16),
            V((NZ, HALF, D), BF16),
            V((NZ, 2, D), BF16),
            V((HALF, D), BF16),
            V((2, D), BF16),
            V((4, HALF, D), BF16),
            V((4, 2, D), BF16),
            dma((3,)),
            dma((6,)), dma((6,)), dma, dma((17,)), dma, dma((20,)), dma, dma((2,)), dma((4,)),
            dma((3,)), dma, dma((2,)), dma, dma((12,)), dma((12,)), dma((9,)),
        ],
        compiler_params=pltpu.CompilerParams(
            collective_id=0, has_side_effects=True, vmem_limit_bytes=66500000),
        name="contrastive",
    )(log_scale, bias, image_embed, text_feature, text_head)
    return pl.pallas_call(
        deliver,
        out_shape=shapes,
        in_specs=[vmem] * 3,
        out_specs=(hbm, hbm, hbm),
        scratch_shapes=[dma((3,))],
        compiler_params=pltpu.CompilerParams(vmem_limit_bytes=2**20),
        name="deliver",
    )(*results)


def solution(mesh):
    both = P(("grp", "blk"), None)
    return jax.shard_map(
        local,
        mesh=mesh,
        in_specs=(both, both, P(), P(), P()),
        out_specs=(both, both, P("blk", None)),
        check_vma=False,
    )
```

```python
import jax
import jax.numpy as jnp
from jax import lax
from jax.experimental import pallas as pl
from jax.experimental.pallas import tpu as pltpu
from jax.sharding import PartitionSpec as P

MESH = pl.DeviceIdType.MESH
EPSILON = 1e-06
F32 = jnp.float32
BF16 = jnp.bfloat16
D = 1152
ROWS = 32
HALF = 16
NX, NY, NZ, NK = 4, 4, 8, 2
COLS = D // NZ
SLICE = 18


def place():
    grp = lax.axis_index("grp")
    blk = lax.axis_index("blk")
    return blk % 4, (grp // 2) * 2 + (blk // 4) % 2, blk // 8, grp % 2


def device(x, y, z, k):
    return ((y // 2) * 2 + k, z * 8 + (y % 2) * 4 + x)


TEXT_ROW = {s: n * ROWS for n, s in enumerate((0, 1, 7, 2, 6, 3, 5, 4))}
TEXTS = 256
IMAGES = 1024
CHUNKS = ((0, 640), (640, 512))
PIECES = ((0, 768), (768, 384))


def rows(start, count):
    return pl.ds(start, count)


def kernel(
    scale_ref, bias_ref, image_hbm, text_hbm, head_hbm,
    gi_ref, gt_ref, gh_ref, image_ref, text_ref, fsel_ref, head, img, txt, wt, tp, ip, rz, iay, iax, iby, ibx,
    ipd, tdir, pall, fall, hp, hm, hl, rm, rl, sm, sl, qm, ql,
    in_sem, r_first, r_second, r_pair, r_z, r_f, r_rs, r_rs1, r_ex, r_ir,
    r_p, r_pk, r_hm, r_hl, s_q, r_q, s_all,
):
    x, y, z, k = place()

    def at(dx=0, dy=0, dz=0, dk=0):
        return device((x + dx) % NX, (y + dy) % NY, (z + dz) % NZ, (k + dk) % NK)

    def send(src, dst, group, rsem, where):
        copy = pltpu.make_async_remote_copy(
            src_ref=src, dst_ref=dst, send_sem=s_all.at[group], recv_sem=rsem,
            device_id=where, device_id_type=MESH,
        )
        copy.start()
        return copy

    def wait_all(ref, sem):
        pltpu.make_async_remote_copy(
            src_ref=ref, dst_ref=ref, send_sem=sem, recv_sem=sem,
            device_id=at(dk=1), device_id_type=MESH,
        ).wait_recv()

    loads = []
    for n, (src, dst) in enumerate((
        (image_hbm, image_ref), (head_hbm, head), (text_hbm, text_ref),
    )):
        loads.append(pltpu.make_async_copy(src, dst, in_sem.at[n]))
        loads[n].start()

    barrier = pltpu.get_barrier_semaphore()
    partners = (
        [dict(dx=i) for i in (1, 2, 3)]
        + [dict(dy=i) for i in (1, 2, 3)]
        + [dict(dz=i) for i in (1, 2, 6, 7)]
        + [dict(dk=1)]
    )
    for p in partners:
        pl.semaphore_signal(barrier, inc=1, device_id=at(**p), device_id_type=MESH)

    loads[0].wait()
    wide = image_ref[...].astype(F32)
    image_len = jnp.sqrt(jnp.sum(wide * wide, axis=-1, keepdims=True) + EPSILON)
    low = (wide / image_len).astype(BF16)
    img[rows(0, HALF), :] = low[:HALF]
    img[rows(256, HALF), :] = low[HALF:]

    pl.semaphore_wait(barrier, len(partners))

    ca, cb = {}, {}

    def sem_of(first, i, j):
        return r_first.at[first * 3 + i - 1] if j == 0 else r_second.at[first * 3 + j - 1]

    def ship_a(tx, ty, sx, where):
        ca[(tx, ty)] = send(img.at[rows(sx * HALF, HALF), :], img.at[rows((ty * 4 + tx) * HALF, HALF), :],
                            0, sem_of(0, tx, ty), where)

    def ship_b(tx, ty, sy, where):
        cb[(tx, ty)] = send(img.at[rows(256 + sy * HALF, HALF), :],
                            img.at[rows(256 + (tx * 4 + ty) * HALF, HALF), :],
                            0, sem_of(1, ty, tx), where)

    def pair(first, j):
        start = first * 256 + j * 64
        if j > 0:
            wait_all(img.at[rows(start, 64), :], r_second.at[first * 3 + j - 1])
        send(img.at[rows(start, 64), :], img.at[rows(512 + start, 64), :], 2, r_pair, at(dk=1))

    order = (1, 3, 2)
    for i in order:
        ship_a(4 - i, 0, 0, at(dx=i))
        ship_b(0, 4 - i, 0, at(dy=i))
    for i in order:
        ship_a(0, 4 - i, 0, at(dy=i))
        ship_b(4 - i, 0, 0, at(dx=i))

    loads[1].wait()
    loads[2].wait()
    projected = jnp.dot(text_ref[...], head[...], preferred_element_type=F32)
    text_len = jnp.sqrt(jnp.sum(projected * projected, axis=-1, keepdims=True) + EPSILON)
    text_dir = projected / text_len
    tdir[...] = text_dir
    txt[rows(0, ROWS), :] = text_dir.astype(BF16)

    cz = {}

    def ship_zc(sign, step, half, c):
        before = min(step - 1, 2)
        src_slot = ((8 - before) % 8) if sign > 0 else before
        dst_slot = (8 - step) if sign > 0 else step
        n = 16 if step > 2 else (((0 if sign > 0 else 2) + step - 1) * 2 + half) * 2 + c
        cz[(sign, step, half, c)] = send(
            txt.at[rows(TEXT_ROW[src_slot] + half * HALF, HALF), pl.ds(*CHUNKS[c])],
            txt.at[rows(TEXT_ROW[dst_slot] + half * HALF, HALF), pl.ds(*CHUNKS[c])],
            1, r_z.at[n], at(dz=sign * (step - before)))

    for half in range(2):
        for c in range(2):
            ship_zc(1, 1, half, c)
            ship_zc(-1, 1, half, c)

    def forward_image(i):
        ca[(i, 0)].wait_recv()
        for j in order:
            ship_a(i, 4 - j, i, at(dy=j))
        cb[(0, i)].wait_recv()
        for j in order:
            ship_b(4 - j, i, i, at(dx=j))

    column = lax.broadcasted_iota(jnp.int32, (1, COLS), 1)
    source = column
    for n in range(1, NZ):
        source = source + jnp.where(column >= n * SLICE, COLS - SLICE, 0)
    entry = lax.broadcasted_iota(jnp.int32, (D, COLS), 0)

    def select(q):
        chosen = jnp.where(entry == source + q * SLICE, 1.0, 0.0).astype(BF16)
        fsel_ref[q] = jnp.dot(text_ref[...], chosen, preferred_element_type=F32).astype(BF16)

    forward_image(3)
    forward_image(1)
    for step in (1, 2):
        for half in range(2):
            for c in range(2):
                for sign in (1, -1):
                    cz[(sign, step, half, c)].wait_recv()
                    if step == 2 and half == (0 if sign > 0 else 1):
                        ship_zc(sign, 4, half, c)
                    ship_zc(sign, step + 1, half, c)
        if step == 1:
            forward_image(2)
            pair(0, 0)
            pair(1, 0)
            pl.loop(0, 4)(select)
    pl.loop(4, 8)(select)
    for j in (1, 3, 2):
        pair(0, j)
        pair(1, j)
    factor = jnp.exp(jnp.full((1, 1), scale_ref[0], F32))
    offset = bias_ref[0]

    def weigh(i, core):
        part = rows(i * 128, 128)
        logits = factor * lax.dot_general(
            txt[part, :], img[rows(core * 512, 512), :], (((1,), (1,)), ((), ())),
            preferred_element_type=F32) + offset
        prob = jax.nn.sigmoid(logits)
        if i == 0 and core == 0:
            row = lax.broadcasted_iota(jnp.int32, (128, 512), 0)
            col = lax.broadcasted_iota(jnp.int32, (128, 512), 1)
            want = jnp.where(row < HALF, row, row + 240)
            prob = prob - jnp.where((row < ROWS) & (col == want), 1.0, 0.0).astype(F32)
        wt[part, pl.ds(core * 512, 512)] = (factor * prob).astype(BF16)

    def tile(i):
        part = rows(i * 128, 128)
        tp[part, :] = jnp.dot(wt[part, :], img[...], preferred_element_type=F32).astype(BF16)

    cr = {}

    def rz_slot(sign, dist, half):
        return ((0 if sign > 0 else 4) + dist - 1) * 2 + half

    def ship_rs(sign, dist, half, c):
        slot = dist if sign > 0 else (8 - dist)
        n = rz_slot(sign, dist, half)
        m = ((0 if sign > 0 else 2) + half) * 2 + c + 4 + 8 * (3 - dist)
        if dist == 4:
            m = (0 if sign > 0 else 2) + c
        cols = pl.ds(*CHUNKS[c])
        cr[(sign, dist, half, c)] = send(
            tp.at[rows(TEXT_ROW[slot] + half * HALF, HALF), cols], rz.at[n, :, cols],
            1, r_rs1 if dist < 3 else r_rs.at[m], at(dz=sign * (2 if dist in (2, 4) else 1)))

    def take_rs(sign, dists, half, c):
        slot = 2 if sign > 0 else 6
        part = rows(TEXT_ROW[slot] + half * HALF, HALF)
        cols = pl.ds(*CHUNKS[c])
        total = tp[part, cols].astype(F32)
        for dist in dists:
            cr[(sign, dist, half, c)].wait_recv()
            total = total + rz[rz_slot(sign, dist, half), :, cols].astype(F32)
        tp[part, cols] = total.astype(BF16)
        ship_rs(sign, 2, half, c)

    def image_tile(i):
        part = rows(i * 256, 256)
        ip[part, :] = lax.dot_general(
            wt[:, part], txt[...], (((0,), (0,)), ((), ())), preferred_element_type=F32).astype(BF16)

    ci = {}

    def ship_ir(name, dist, src, dst, n, where):
        ci[(name, dist)] = send(src, dst, 4, r_ir.at[n], where)

    def give_image(first):
        image_tile(2 + first)
        return send(ip.at[rows(512 + first * 256, 256), :], ipd.at[rows(first * 256, 256), :],
                    3, r_ex.at[first], at(dk=1))

    def join_image(first, copy):
        copy.wait_recv()

        def add(j):
            part = rows(pl.multiple_of(first * 256 + j * ROWS, ROWS), ROWS)
            ip[part, :] = (ip[part, :].astype(F32) + ipd[part, :].astype(F32)).astype(BF16)

        pl.loop(0, 8)(add)

    weigh(0, 0)
    wait_all(txt.at[rows(0, 96), :], r_z.at[16])
    weigh(1, 0)
    wait_all(img.at[rows(512, 512), :], r_pair)
    weigh(1, 1)
    tile(1)
    for c in range(2):
        ship_rs(1, 4, 0, c)
        ship_rs(-1, 4, 1, c)
        for half in range(2):
            ship_rs(1, 3, half, c)
            ship_rs(-1, 3, half, c)
    weigh(0, 1)
    tile(0)
    for c in range(2):
        for half in range(2):
            ship_rs(1, 1, half, c)
            ship_rs(-1, 1, half, c)
    ex = [give_image(0), give_image(1)]
    image_tile(0)
    image_tile(1)
    for c in range(2):
        take_rs(1, (4, 3), 0, c)
        take_rs(-1, (4, 3), 1, c)
        take_rs(1, (3,), 1, c)
        take_rs(-1, (3,), 0, c)
    join_image(0, ex[0])
    for i in order:
        ship_ir("ay", i, ip.at[rows(i * 64, 64), :], iay.at[i - 1], 0, at(dy=i))
    join_image(1, ex[1])
    for i in order:
        for j in range(4):
            ship_ir("by", i, ip.at[rows(256 + j * 64 + i * HALF, HALF), :],
                    iby.at[i - 1, rows(j * HALF, HALF), :], 1, at(dy=i))
    fall[0] = fsel_ref[k * 4 + x]
    for dk in range(2):
        for dx in range(4):
            if dk == 0 and dx == 0:
                continue
            slot = ((4 - dx) % 4) + 4 * dk
            send(fsel_ref.at[((k + dk) % 2) * 4 + (x + dx) % 4], fall.at[slot], 6, r_f, at(dx=dx, dk=dk))

    def fold(base, step, recv, sem):
        wait_all(recv, sem)
        for j in range(4):
            part = rows(base + j * step, HALF)
            total = ip[part, :].astype(F32)
            for i in range(3):
                total = total + recv[i, rows(j * HALF, HALF), :].astype(F32)
            ip[part, :] = total.astype(BF16)

    wait_all(rz.at[pl.ds(0, 8)], r_rs1)
    halves = []
    for half in range(2):
        total = tp[rows(half * HALF, HALF), :].astype(F32)
        for dist in (1, 2):
            for sign in (1, -1):
                total = total + rz[rz_slot(sign, dist, half)].astype(F32)
        halves.append(total)
    text_sum = jnp.concatenate(halves, axis=0)
    text_dir = tdir[...]
    proj_grad = (
        (text_sum - text_dir * jnp.sum(text_dir * text_sum, axis=-1, keepdims=True)) / text_len
    ).astype(BF16)
    pall[0] = proj_grad

    cp = {}
    for dx in order:
        slot = 4 - dx
        cp[slot] = send(pall.at[0], pall.at[slot], 5, r_p.at[slot - 1], at(dx=dx))
    send(pall.at[0], pall.at[4], 5, r_pk, at(dk=1))

    gt_ref[...] = lax.dot_general(
        proj_grad, head[...], (((1,), (1,)), ((), ())), preferred_element_type=F32).astype(BF16)

    for slot in (1, 3, 2):
        cp[slot].wait_recv()
        send(pall.at[slot], pall.at[4 + slot], 5, r_pk, at(dk=1))
    wait_all(pall.at[pl.ds(4, 4)], r_pk)
    wait_all(fall.at[pl.ds(1, 7)], r_f)

    hp[...] = lax.dot_general(
        fall[...].reshape(256, COLS), pall[...].reshape(256, D), (((0,), (0,)), ((), ())),
        preferred_element_type=F32)
    for s in range(NZ):
        part = hp[rows(s * SLICE, SLICE), :]
        hm[s] = part[:HALF].astype(BF16)
        hl[s] = part[HALF:].astype(BF16)
    far = (4, 3, 5, 2, 6, 1, 7)
    for c in range(2):
        cols = pl.ds(*PIECES[c])
        for dz in far:
            dest = (z + dz) % NZ
            send(hm.at[dest, :, cols], rm.at[dz, :, cols], 7, r_hm.at[c], at(dz=dz))
            if c == 0:
                send(hl.at[dest], rl.at[dz], 8, r_hl, at(dz=dz))

    fold(0, HALF, iay, r_ir.at[0])
    fold(256, 64, iby, r_ir.at[1])
    for i in order:
        ship_ir("ax", i, ip.at[rows(i * HALF, HALF), :], iax.at[i - 1], 2, at(dx=i))
        ship_ir("bx", i, ip.at[rows(256 + i * 64, HALF), :], ibx.at[i - 1], 3, at(dx=i))
    y_lo = y % 2

    def piece(p, slot):
        if p == 2:
            return sl, ql.at[slot]
        return sm.at[:, pl.ds(*PIECES[p])], qm.at[slot, :, pl.ds(*PIECES[p])]

    def final(p, target_y, target_k, slot):
        src, dst = piece(p, slot)
        return pltpu.make_async_remote_copy(
            src_ref=src, dst_ref=dst, send_sem=s_q.at[p * 4 + target_y // 2 * 2 + target_k],
            recv_sem=r_q.at[p * 4 + slot], device_id=device(x, target_y, z, target_k), device_id_type=MESH)

    def scatter(pieces):
        for h in range(2):
            for tk in range(2):
                ty = k + 2 * h
                own = (ty == y) & (tk == k)

                @pl.when(jnp.logical_not(own))
                def _():
                    for p in pieces:
                        final(p, ty, tk, y).start()

                @pl.when(own)
                def _():
                    for p in pieces:
                        src, dst = piece(p, y)
                        dst[...] = src[...]

    def collect(pieces):
        for sy in range(4):
            @pl.when(jnp.logical_not((sy == y) & (k == y_lo)))
            def _():
                for p in pieces:
                    final(p, y, k, sy).wait_recv()

    def sum_z(own, recv):
        total = own.astype(F32)
        for dz in far:
            total = total + recv(dz).astype(F32)
        return total.astype(BF16)

    def sum_y(part):
        total = part(0).astype(F32)
        for sy in range(1, 4):
            total = total + part(sy).astype(F32)
        return total

    def finish_image():
        wait_all(iax, r_ir.at[2])
        wait_all(ibx, r_ir.at[3])
        total_a = ip[rows(0, HALF), :].astype(F32)
        total_b = ip[rows(256, HALF), :].astype(F32)
        for i in range(3):
            total_a = total_a + iax[i].astype(F32)
            total_b = total_b + ibx[i].astype(F32)
        image_sum = jnp.concatenate([total_a, total_b], axis=0)
        wide = image_ref[...].astype(F32)
        image_len = jnp.sqrt(jnp.sum(wide * wide, axis=-1, keepdims=True) + EPSILON)
        image_dir = wide / image_len
        gi_ref[...] = (
            (image_sum - image_dir * jnp.sum(image_dir * image_sum, axis=-1, keepdims=True)) / image_len
        ).astype(BF16)

    for c in range(2):
        cols = pl.ds(*PIECES[c])
        wait_all(rm.at[pl.ds(1, 7), :, cols], r_hm.at[c])
        sm[:, cols] = sum_z(hm[z, :, cols], lambda dz: rm[dz, :, cols])
        if c == 0:
            wait_all(rl.at[pl.ds(1, 7)], r_hl)
            sl[...] = sum_z(hl[z], lambda dz: rl[dz])
        scatter((0, 2) if c == 0 else (1,))
        if c == 0:
            finish_image()
    for c in range(2):
        cols = pl.ds(*PIECES[c])
        collect((0, 2) if c == 0 else (1,))
        gh_ref[pl.ds(0, HALF), cols] = sum_y(lambda sy: qm[sy, :, cols])
        if c == 0:
            gh_ref[pl.ds(HALF, 2), :] = sum_y(lambda sy: ql[sy])

    for n, ref in enumerate((
        img.at[rows(0, 480), :],
        img.at[rows(0, 448), :],
        img.at[rows(0, 512), :],
        img.at[rows(0, 512), :],
        img.at[rows(0, 480), :],
        pall.at[pl.ds(0, 7)],
        fall.at[pl.ds(0, 7)],
        rm.at[pl.ds(0, 7)],
        rl.at[pl.ds(0, 7)],
    )):
        wait_all(ref, s_all.at[n])
    for h in range(2):
        for tk in range(2):
            ty = k + 2 * h

            @pl.when(jnp.logical_not((ty == y) & (tk == k)))
            def _():
                for p in range(3):
                    final(p, ty, tk, y).wait_send()


def deliver(gi_ref, gt_ref, gh_ref, gi_out, gt_out, gh_out, sem):
    copies = [
        pltpu.make_async_copy(src, dst, sem.at[n])
        for n, (src, dst) in enumerate(((gi_ref, gi_out), (gt_ref, gt_out), (gh_ref, gh_out)))
    ]
    for copy in copies:
        copy.start()
    for copy in copies:
        copy.wait()


def local(image_embed, text_feature, text_head, log_scale, bias):
    hbm = pl.BlockSpec(memory_space=pltpu.HBM)
    vmem = pl.BlockSpec(memory_space=pltpu.VMEM)
    dma = pltpu.SemaphoreType.DMA
    V = pltpu.VMEM
    shapes = (
        jax.ShapeDtypeStruct((ROWS, D), BF16),
        jax.ShapeDtypeStruct((ROWS, D), BF16),
        jax.ShapeDtypeStruct((SLICE, D), F32),
    )
    results = pl.pallas_call(
        kernel,
        out_shape=tuple(pltpu.VMEM(a.shape, a.dtype) for a in shapes),
        in_specs=[pl.BlockSpec(memory_space=pltpu.SMEM)] * 2 + [hbm] * 3,
        out_specs=(vmem, vmem, vmem),
        scratch_shapes=[
            V((ROWS, D), BF16),
            V((ROWS, D), BF16),
            V((8, ROWS, COLS), BF16),
            V((D, D), BF16),
            V((IMAGES, D), BF16),
            V((TEXTS, D), BF16),
            V((TEXTS, IMAGES), BF16),
            V((TEXTS, D), BF16),
            V((IMAGES, D), BF16),
            V((16, HALF, D), BF16),
            V((3, 64, D), BF16),
            V((3, HALF, D), BF16),
            V((3, 64, D), BF16),
            V((3, HALF, D), BF16),
            V((512, D), BF16),
            V((ROWS, D), F32),
            V((8, ROWS, D), BF16),
            V((8, ROWS, COLS), BF16),
            V((COLS, D), F32),
            V((NZ, HALF, D), BF16),
            V((NZ, 2, D), BF16),
            V((NZ, HALF, D), BF16),
            V((NZ, 2, D), BF16),
            V((HALF, D), BF16),
            V((2, D), BF16),
            V((4, HALF, D), BF16),
            V((4, 2, D), BF16),
            dma((3,)),
            dma((6,)), dma((6,)), dma, dma((17,)), dma, dma((12,)), dma, dma((2,)), dma((4,)),
            dma((3,)), dma, dma((2,)), dma, dma((12,)), dma((12,)), dma((9,)),
        ],
        compiler_params=pltpu.CompilerParams(
            collective_id=0, has_side_effects=True, vmem_limit_bytes=66500000),
        name="contrastive",
    )(log_scale, bias, image_embed, text_feature, text_head)
    return pl.pallas_call(
        deliver,
        out_shape=shapes,
        in_specs=[vmem] * 3,
        out_specs=(hbm, hbm, hbm),
        scratch_shapes=[dma((3,))],
        compiler_params=pltpu.CompilerParams(vmem_limit_bytes=2**20),
        name="deliver",
    )(*results)


def solution(mesh):
    both = P(("grp", "blk"), None)
    return jax.shard_map(
        local,
        mesh=mesh,
        in_specs=(both, both, P(), P(), P()),
        out_specs=(both, both, P("blk", None)),
        check_vma=False,
    )
```

```python
import jax
import jax.numpy as jnp
from jax import lax
from jax.experimental import pallas as pl
from jax.experimental.pallas import tpu as pltpu
from jax.sharding import PartitionSpec as P

MESH = pl.DeviceIdType.MESH
EPSILON = 1e-06
F32 = jnp.float32
BF16 = jnp.bfloat16
D = 1152
ROWS = 32
HALF = 16
NX, NY, NZ, NK = 4, 4, 8, 2
COLS = D // NZ
SLICE = 18


def place():
    grp = lax.axis_index("grp")
    blk = lax.axis_index("blk")
    return blk % 4, (grp // 2) * 2 + (blk // 4) % 2, blk // 8, grp % 2


def device(x, y, z, k):
    return ((y // 2) * 2 + k, z * 8 + (y % 2) * 4 + x)


TEXT_ROW = {s: n * ROWS for n, s in enumerate((0, 1, 7, 2, 6, 3, 5, 4))}
TEXTS = 256
IMAGES = 1024
CHUNKS = ((0, 640), (640, 512))
PIECES = ((0, 768), (768, 384))


def rows(start, count):
    return pl.ds(start, count)


def kernel(
    scale_ref, bias_ref, image_hbm, text_hbm, head_hbm,
    gi_ref, gt_ref, gh_ref, image_ref, text_ref, fsel_ref, head, img, txt, wt, tp, ip, rz, iay, iax, iby, ibx,
    ipd, tdir, pall, fall, hp, hm, hl, rm, rl, sm, sl, qm, ql,
    in_sem, r_first, r_second, r_pair, r_z, r_f, r_rs, r_rs1, r_ex, r_ir,
    r_p, r_pk, r_hm, r_hl, s_q, r_q, s_all,
):
    x, y, z, k = place()

    def at(dx=0, dy=0, dz=0, dk=0):
        return device((x + dx) % NX, (y + dy) % NY, (z + dz) % NZ, (k + dk) % NK)

    def send(src, dst, group, rsem, where):
        copy = pltpu.make_async_remote_copy(
            src_ref=src, dst_ref=dst, send_sem=s_all.at[group], recv_sem=rsem,
            device_id=where, device_id_type=MESH,
        )
        copy.start()
        return copy

    def wait_all(ref, sem):
        pltpu.make_async_remote_copy(
            src_ref=ref, dst_ref=ref, send_sem=sem, recv_sem=sem,
            device_id=at(dk=1), device_id_type=MESH,
        ).wait_recv()

    loads = []
    for n, (src, dst) in enumerate((
        (image_hbm, image_ref), (head_hbm, head), (text_hbm, text_ref),
    )):
        loads.append(pltpu.make_async_copy(src, dst, in_sem.at[n]))
        loads[n].start()

    barrier = pltpu.get_barrier_semaphore()
    partners = (
        [dict(dx=i) for i in (1, 2, 3)]
        + [dict(dy=i) for i in (1, 2, 3)]
        + [dict(dz=i) for i in (1, 2, 6, 7)]
        + [dict(dk=1)]
    )
    for p in partners:
        pl.semaphore_signal(barrier, inc=1, device_id=at(**p), device_id_type=MESH)

    loads[0].wait()
    wide = image_ref[...].astype(F32)
    image_len = jnp.sqrt(jnp.sum(wide * wide, axis=-1, keepdims=True) + EPSILON)
    low = (wide / image_len).astype(BF16)
    img[rows(0, HALF), :] = low[:HALF]
    img[rows(256, HALF), :] = low[HALF:]

    pl.semaphore_wait(barrier, len(partners))

    ca, cb = {}, {}

    def sem_of(first, i, j):
        return r_first.at[first * 3 + i - 1] if j == 0 else r_second.at[first * 3 + j - 1]

    def ship_a(tx, ty, sx, where):
        ca[(tx, ty)] = send(img.at[rows(sx * HALF, HALF), :], img.at[rows((ty * 4 + tx) * HALF, HALF), :],
                            0, sem_of(0, tx, ty), where)

    def ship_b(tx, ty, sy, where):
        cb[(tx, ty)] = send(img.at[rows(256 + sy * HALF, HALF), :],
                            img.at[rows(256 + (tx * 4 + ty) * HALF, HALF), :],
                            0, sem_of(1, ty, tx), where)

    def pair(first, j):
        start = first * 256 + j * 64
        if j > 0:
            wait_all(img.at[rows(start, 64), :], r_second.at[first * 3 + j - 1])
        send(img.at[rows(start, 64), :], img.at[rows(512 + start, 64), :], 2, r_pair, at(dk=1))

    order = (1, 3, 2)
    for i in order:
        ship_a(4 - i, 0, 0, at(dx=i))
        ship_b(0, 4 - i, 0, at(dy=i))
    for i in order:
        ship_a(0, 4 - i, 0, at(dy=i))
        ship_b(4 - i, 0, 0, at(dx=i))

    loads[1].wait()
    loads[2].wait()
    projected = jnp.dot(text_ref[...], head[...], preferred_element_type=F32)
    text_len = jnp.sqrt(jnp.sum(projected * projected, axis=-1, keepdims=True) + EPSILON)
    text_dir = projected / text_len
    tdir[...] = text_dir
    txt[rows(0, ROWS), :] = text_dir.astype(BF16)

    cz = {}

    def ship_zc(sign, step, half, c):
        before = min(step - 1, 2)
        src_slot = ((8 - before) % 8) if sign > 0 else before
        dst_slot = (8 - step) if sign > 0 else step
        n = 16 if step > 2 else (((0 if sign > 0 else 2) + step - 1) * 2 + half) * 2 + c
        cz[(sign, step, half, c)] = send(
            txt.at[rows(TEXT_ROW[src_slot] + half * HALF, HALF), pl.ds(*CHUNKS[c])],
            txt.at[rows(TEXT_ROW[dst_slot] + half * HALF, HALF), pl.ds(*CHUNKS[c])],
            1, r_z.at[n], at(dz=sign * (step - before)))

    for half in range(2):
        for c in range(2):
            ship_zc(1, 1, half, c)
            ship_zc(-1, 1, half, c)

    def forward_image(i):
        ca[(i, 0)].wait_recv()
        for j in order:
            ship_a(i, 4 - j, i, at(dy=j))
        cb[(0, i)].wait_recv()
        for j in order:
            ship_b(4 - j, i, i, at(dx=j))

    column = lax.broadcasted_iota(jnp.int32, (1, COLS), 1)
    source = column
    for n in range(1, NZ):
        source = source + jnp.where(column >= n * SLICE, COLS - SLICE, 0)
    entry = lax.broadcasted_iota(jnp.int32, (D, COLS), 0)

    def select(q):
        chosen = jnp.where(entry == source + q * SLICE, 1.0, 0.0).astype(BF16)
        fsel_ref[q] = jnp.dot(text_ref[...], chosen, preferred_element_type=F32).astype(BF16)

    forward_image(3)
    forward_image(1)
    for step in (1, 2):
        for half in range(2):
            for c in range(2):
                for sign in (1, -1):
                    cz[(sign, step, half, c)].wait_recv()
                    if step == 2 and half == (0 if sign > 0 else 1):
                        ship_zc(sign, 4, half, c)
                    ship_zc(sign, step + 1, half, c)
        if step == 1:
            forward_image(2)
            pair(0, 0)
            pair(1, 0)
            pl.loop(0, 4)(select)
    pl.loop(4, 8)(select)
    for j in (1, 3, 2):
        pair(0, j)
        pair(1, j)
    factor = jnp.exp(jnp.full((1, 1), scale_ref[0], F32))
    offset = bias_ref[0]

    def weigh(i, core):
        part = rows(i * 128, 128)
        logits = factor * lax.dot_general(
            txt[part, :], img[rows(core * 512, 512), :], (((1,), (1,)), ((), ())),
            preferred_element_type=F32) + offset
        prob = jax.nn.sigmoid(logits)
        if i == 0 and core == 0:
            row = lax.broadcasted_iota(jnp.int32, (128, 512), 0)
            col = lax.broadcasted_iota(jnp.int32, (128, 512), 1)
            want = jnp.where(row < HALF, row, row + 240)
            prob = prob - jnp.where((row < ROWS) & (col == want), 1.0, 0.0).astype(F32)
        wt[part, pl.ds(core * 512, 512)] = (factor * prob).astype(BF16)

    def tile(i):
        part = rows(i * 128, 128)
        tp[part, :] = jnp.dot(wt[part, :], img[...], preferred_element_type=F32).astype(BF16)

    cr = {}

    def rz_slot(sign, dist, half):
        return ((0 if sign > 0 else 4) + dist - 1) * 2 + half

    def ship_rs(sign, dist, half, c):
        slot = dist if sign > 0 else (8 - dist)
        n = rz_slot(sign, dist, half)
        m = ((0 if sign > 0 else 2) + half) * 2 + c + 4 + 8 * (3 - dist)
        if dist == 4:
            m = (0 if sign > 0 else 2) + c
        cols = pl.ds(*CHUNKS[c])
        cr[(sign, dist, half, c)] = send(
            tp.at[rows(TEXT_ROW[slot] + half * HALF, HALF), cols], rz.at[n, :, cols],
            1, r_rs1 if dist < 3 else r_rs.at[m], at(dz=sign * (2 if dist in (2, 4) else 1)))

    def take_rs(sign, dists, half, c):
        slot = 2 if sign > 0 else 6
        part = rows(TEXT_ROW[slot] + half * HALF, HALF)
        cols = pl.ds(*CHUNKS[c])
        total = tp[part, cols].astype(F32)
        for dist in dists:
            cr[(sign, dist, half, c)].wait_recv()
            total = total + rz[rz_slot(sign, dist, half), :, cols].astype(F32)
        tp[part, cols] = total.astype(BF16)
        ship_rs(sign, 2, half, c)

    def image_tile(i):
        part = rows(i * 256, 256)
        ip[part, :] = lax.dot_general(
            wt[:, part], txt[...], (((0,), (0,)), ((), ())), preferred_element_type=F32).astype(BF16)

    ci = {}

    def ship_ir(name, dist, src, dst, n, where):
        ci[(name, dist)] = send(src, dst, 4, r_ir.at[n], where)

    def give_image(first):
        image_tile(2 + first)
        return send(ip.at[rows(512 + first * 256, 256), :], ipd.at[rows(first * 256, 256), :],
                    3, r_ex.at[first], at(dk=1))

    def join_image(first, copy):
        copy.wait_recv()

        def add(j):
            part = rows(pl.multiple_of(first * 256 + j * ROWS, ROWS), ROWS)
            ip[part, :] = (ip[part, :].astype(F32) + ipd[part, :].astype(F32)).astype(BF16)

        pl.loop(0, 8)(add)

    weigh(0, 0)
    wait_all(txt.at[rows(0, 96), :], r_z.at[16])
    weigh(1, 0)
    wait_all(img.at[rows(512, 512), :], r_pair)
    weigh(1, 1)
    tile(1)
    for c in range(2):
        ship_rs(1, 3, 1, c)
        ship_rs(-1, 3, 0, c)
        ship_rs(1, 4, 0, c)
        ship_rs(-1, 4, 1, c)
        ship_rs(1, 3, 0, c)
        ship_rs(-1, 3, 1, c)
    weigh(0, 1)
    tile(0)
    for c in range(2):
        for half in range(2):
            ship_rs(1, 1, half, c)
            ship_rs(-1, 1, half, c)
    ex = [give_image(0), give_image(1)]
    image_tile(0)
    image_tile(1)
    for c in range(2):
        take_rs(1, (3,), 1, c)
        take_rs(-1, (3,), 0, c)
        take_rs(1, (4, 3), 0, c)
        take_rs(-1, (4, 3), 1, c)
    join_image(0, ex[0])
    for i in order:
        ship_ir("ay", i, ip.at[rows(i * 64, 64), :], iay.at[i - 1], 0, at(dy=i))
    join_image(1, ex[1])
    for i in order:
        for j in range(4):
            ship_ir("by", i, ip.at[rows(256 + j * 64 + i * HALF, HALF), :],
                    iby.at[i - 1, rows(j * HALF, HALF), :], 1, at(dy=i))
    fall[0] = fsel_ref[k * 4 + x]
    for dk in range(2):
        for dx in range(4):
            if dk == 0 and dx == 0:
                continue
            slot = ((4 - dx) % 4) + 4 * dk
            send(fsel_ref.at[((k + dk) % 2) * 4 + (x + dx) % 4], fall.at[slot], 6, r_f, at(dx=dx, dk=dk))

    def fold(base, step, recv, sem):
        wait_all(recv, sem)
        for j in range(4):
            part = rows(base + j * step, HALF)
            total = ip[part, :].astype(F32)
            for i in range(3):
                total = total + recv[i, rows(j * HALF, HALF), :].astype(F32)
            ip[part, :] = total.astype(BF16)

    wait_all(rz.at[pl.ds(0, 8)], r_rs1)
    halves = []
    for half in range(2):
        total = tp[rows(half * HALF, HALF), :].astype(F32)
        for dist in (1, 2):
            for sign in (1, -1):
                total = total + rz[rz_slot(sign, dist, half)].astype(F32)
        halves.append(total)
    text_sum = jnp.concatenate(halves, axis=0)
    text_dir = tdir[...]
    proj_grad = (
        (text_sum - text_dir * jnp.sum(text_dir * text_sum, axis=-1, keepdims=True)) / text_len
    ).astype(BF16)
    pall[0] = proj_grad

    cp = {}
    for dx in order:
        slot = 4 - dx
        cp[slot] = send(pall.at[0], pall.at[slot], 5, r_p.at[slot - 1], at(dx=dx))
    send(pall.at[0], pall.at[4], 5, r_pk, at(dk=1))

    gt_ref[...] = lax.dot_general(
        proj_grad, head[...], (((1,), (1,)), ((), ())), preferred_element_type=F32).astype(BF16)

    for slot in (1, 3, 2):
        cp[slot].wait_recv()
        send(pall.at[slot], pall.at[4 + slot], 5, r_pk, at(dk=1))
    wait_all(pall.at[pl.ds(4, 4)], r_pk)
    wait_all(fall.at[pl.ds(1, 7)], r_f)

    hp[...] = lax.dot_general(
        fall[...].reshape(256, COLS), pall[...].reshape(256, D), (((0,), (0,)), ((), ())),
        preferred_element_type=F32)
    for s in range(NZ):
        part = hp[rows(s * SLICE, SLICE), :]
        hm[s] = part[:HALF].astype(BF16)
        hl[s] = part[HALF:].astype(BF16)
    far = (4, 3, 5, 2, 6, 1, 7)
    for c in range(2):
        cols = pl.ds(*PIECES[c])
        for dz in far:
            dest = (z + dz) % NZ
            send(hm.at[dest, :, cols], rm.at[dz, :, cols], 7, r_hm.at[c], at(dz=dz))
            if c == 0:
                send(hl.at[dest], rl.at[dz], 8, r_hl, at(dz=dz))

    fold(0, HALF, iay, r_ir.at[0])
    fold(256, 64, iby, r_ir.at[1])
    for i in order:
        ship_ir("ax", i, ip.at[rows(i * HALF, HALF), :], iax.at[i - 1], 2, at(dx=i))
        ship_ir("bx", i, ip.at[rows(256 + i * 64, HALF), :], ibx.at[i - 1], 3, at(dx=i))
    y_lo = y % 2

    def piece(p, slot):
        if p == 2:
            return sl, ql.at[slot]
        return sm.at[:, pl.ds(*PIECES[p])], qm.at[slot, :, pl.ds(*PIECES[p])]

    def final(p, target_y, target_k, slot):
        src, dst = piece(p, slot)
        return pltpu.make_async_remote_copy(
            src_ref=src, dst_ref=dst, send_sem=s_q.at[p * 4 + target_y // 2 * 2 + target_k],
            recv_sem=r_q.at[p * 4 + slot], device_id=device(x, target_y, z, target_k), device_id_type=MESH)

    def scatter(pieces):
        for h in range(2):
            for tk in range(2):
                ty = k + 2 * h
                own = (ty == y) & (tk == k)

                @pl.when(jnp.logical_not(own))
                def _():
                    for p in pieces:
                        final(p, ty, tk, y).start()

                @pl.when(own)
                def _():
                    for p in pieces:
                        src, dst = piece(p, y)
                        dst[...] = src[...]

    def collect(pieces):
        for sy in range(4):
            @pl.when(jnp.logical_not((sy == y) & (k == y_lo)))
            def _():
                for p in pieces:
                    final(p, y, k, sy).wait_recv()

    def sum_z(own, recv):
        total = own.astype(F32)
        for dz in far:
            total = total + recv(dz).astype(F32)
        return total.astype(BF16)

    def sum_y(part):
        total = part(0).astype(F32)
        for sy in range(1, 4):
            total = total + part(sy).astype(F32)
        return total

    def finish_image():
        wait_all(iax, r_ir.at[2])
        wait_all(ibx, r_ir.at[3])
        total_a = ip[rows(0, HALF), :].astype(F32)
        total_b = ip[rows(256, HALF), :].astype(F32)
        for i in range(3):
            total_a = total_a + iax[i].astype(F32)
            total_b = total_b + ibx[i].astype(F32)
        image_sum = jnp.concatenate([total_a, total_b], axis=0)
        wide = image_ref[...].astype(F32)
        image_len = jnp.sqrt(jnp.sum(wide * wide, axis=-1, keepdims=True) + EPSILON)
        image_dir = wide / image_len
        gi_ref[...] = (
            (image_sum - image_dir * jnp.sum(image_dir * image_sum, axis=-1, keepdims=True)) / image_len
        ).astype(BF16)

    for c in range(2):
        cols = pl.ds(*PIECES[c])
        wait_all(rm.at[pl.ds(1, 7), :, cols], r_hm.at[c])
        sm[:, cols] = sum_z(hm[z, :, cols], lambda dz: rm[dz, :, cols])
        if c == 0:
            wait_all(rl.at[pl.ds(1, 7)], r_hl)
            sl[...] = sum_z(hl[z], lambda dz: rl[dz])
        scatter((0, 2) if c == 0 else (1,))
        if c == 0:
            finish_image()
    for c in range(2):
        cols = pl.ds(*PIECES[c])
        collect((0, 2) if c == 0 else (1,))
        gh_ref[pl.ds(0, HALF), cols] = sum_y(lambda sy: qm[sy, :, cols])
        if c == 0:
            gh_ref[pl.ds(HALF, 2), :] = sum_y(lambda sy: ql[sy])

    for n, ref in enumerate((
        img.at[rows(0, 480), :],
        img.at[rows(0, 448), :],
        img.at[rows(0, 512), :],
        img.at[rows(0, 512), :],
        img.at[rows(0, 480), :],
        pall.at[pl.ds(0, 7)],
        fall.at[pl.ds(0, 7)],
        rm.at[pl.ds(0, 7)],
        rl.at[pl.ds(0, 7)],
    )):
        wait_all(ref, s_all.at[n])
    for h in range(2):
        for tk in range(2):
            ty = k + 2 * h

            @pl.when(jnp.logical_not((ty == y) & (tk == k)))
            def _():
                for p in range(3):
                    final(p, ty, tk, y).wait_send()


def deliver(gi_ref, gt_ref, gh_ref, gi_out, gt_out, gh_out, sem):
    copies = [
        pltpu.make_async_copy(src, dst, sem.at[n])
        for n, (src, dst) in enumerate(((gi_ref, gi_out), (gt_ref, gt_out), (gh_ref, gh_out)))
    ]
    for copy in copies:
        copy.start()
    for copy in copies:
        copy.wait()


def local(image_embed, text_feature, text_head, log_scale, bias):
    hbm = pl.BlockSpec(memory_space=pltpu.HBM)
    vmem = pl.BlockSpec(memory_space=pltpu.VMEM)
    dma = pltpu.SemaphoreType.DMA
    V = pltpu.VMEM
    shapes = (
        jax.ShapeDtypeStruct((ROWS, D), BF16),
        jax.ShapeDtypeStruct((ROWS, D), BF16),
        jax.ShapeDtypeStruct((SLICE, D), F32),
    )
    results = pl.pallas_call(
        kernel,
        out_shape=tuple(pltpu.VMEM(a.shape, a.dtype) for a in shapes),
        in_specs=[pl.BlockSpec(memory_space=pltpu.SMEM)] * 2 + [hbm] * 3,
        out_specs=(vmem, vmem, vmem),
        scratch_shapes=[
            V((ROWS, D), BF16),
            V((ROWS, D), BF16),
            V((8, ROWS, COLS), BF16),
            V((D, D), BF16),
            V((IMAGES, D), BF16),
            V((TEXTS, D), BF16),
            V((TEXTS, IMAGES), BF16),
            V((TEXTS, D), BF16),
            V((IMAGES, D), BF16),
            V((16, HALF, D), BF16),
            V((3, 64, D), BF16),
            V((3, HALF, D), BF16),
            V((3, 64, D), BF16),
            V((3, HALF, D), BF16),
            V((512, D), BF16),
            V((ROWS, D), F32),
            V((8, ROWS, D), BF16),
            V((8, ROWS, COLS), BF16),
            V((COLS, D), F32),
            V((NZ, HALF, D), BF16),
            V((NZ, 2, D), BF16),
            V((NZ, HALF, D), BF16),
            V((NZ, 2, D), BF16),
            V((HALF, D), BF16),
            V((2, D), BF16),
            V((4, HALF, D), BF16),
            V((4, 2, D), BF16),
            dma((3,)),
            dma((6,)), dma((6,)), dma, dma((17,)), dma, dma((12,)), dma, dma((2,)), dma((4,)),
            dma((3,)), dma, dma((2,)), dma, dma((12,)), dma((12,)), dma((9,)),
        ],
        compiler_params=pltpu.CompilerParams(
            collective_id=0, has_side_effects=True, vmem_limit_bytes=66500000),
        name="contrastive",
    )(log_scale, bias, image_embed, text_feature, text_head)
    return pl.pallas_call(
        deliver,
        out_shape=shapes,
        in_specs=[vmem] * 3,
        out_specs=(hbm, hbm, hbm),
        scratch_shapes=[dma((3,))],
        compiler_params=pltpu.CompilerParams(vmem_limit_bytes=2**20),
        name="deliver",
    )(*results)


def solution(mesh):
    both = P(("grp", "blk"), None)
    return jax.shard_map(
        local,
        mesh=mesh,
        in_specs=(both, both, P(), P(), P()),
        out_specs=(both, both, P("blk", None)),
        check_vma=False,
    )
```

```python
import jax
import jax.numpy as jnp
from jax import lax
from jax.experimental import pallas as pl
from jax.experimental.pallas import tpu as pltpu
from jax.sharding import PartitionSpec as P

MESH = pl.DeviceIdType.MESH
EPSILON = 1e-06
F32 = jnp.float32
BF16 = jnp.bfloat16
D = 1152
ROWS = 32
HALF = 16
NX, NY, NZ, NK = 4, 4, 8, 2
COLS = D // NZ
SLICE = 18


def place():
    grp = lax.axis_index("grp")
    blk = lax.axis_index("blk")
    return blk % 4, (grp // 2) * 2 + (blk // 4) % 2, blk // 8, grp % 2


def device(x, y, z, k):
    return ((y // 2) * 2 + k, z * 8 + (y % 2) * 4 + x)


TEXT_ROW = {s: n * ROWS for n, s in enumerate((0, 1, 7, 2, 6, 3, 5, 4))}
TEXTS = 256
IMAGES = 1024
CHUNKS = ((0, 640), (640, 512))
PIECES = ((0, 768), (768, 384))


def rows(start, count):
    return pl.ds(start, count)


def kernel(
    scale_ref, bias_ref, image_hbm, text_hbm, head_hbm,
    gi_ref, gt_ref, gh_ref, image_ref, text_ref, fsel_ref, head, img, txt, wt, tp, ip, rz, iay, iax, iby, ibx,
    ipd, tdir, pall, fall, hp, hm, hl, rm, rl, sm, sl, qm, ql,
    in_sem, r_first, r_second, r_pair, r_z, r_f, r_rs, r_rs1, r_ex, r_ir,
    r_p, r_pk, r_hm, r_hl, s_q, r_q, s_all,
):
    x, y, z, k = place()

    def at(dx=0, dy=0, dz=0, dk=0):
        return device((x + dx) % NX, (y + dy) % NY, (z + dz) % NZ, (k + dk) % NK)

    def send(src, dst, group, rsem, where):
        copy = pltpu.make_async_remote_copy(
            src_ref=src, dst_ref=dst, send_sem=s_all.at[group], recv_sem=rsem,
            device_id=where, device_id_type=MESH,
        )
        copy.start()
        return copy

    def wait_all(ref, sem):
        pltpu.make_async_remote_copy(
            src_ref=ref, dst_ref=ref, send_sem=sem, recv_sem=sem,
            device_id=at(dk=1), device_id_type=MESH,
        ).wait_recv()

    loads = []
    for n, (src, dst) in enumerate((
        (image_hbm, image_ref), (head_hbm, head), (text_hbm, text_ref),
    )):
        loads.append(pltpu.make_async_copy(src, dst, in_sem.at[n]))
        loads[n].start()

    barrier = pltpu.get_barrier_semaphore()
    partners = (
        [dict(dx=i) for i in (1, 2, 3)]
        + [dict(dy=i) for i in (1, 2, 3)]
        + [dict(dz=i) for i in (1, 2, 6, 7)]
        + [dict(dk=1)]
    )
    for p in partners:
        pl.semaphore_signal(barrier, inc=1, device_id=at(**p), device_id_type=MESH)

    loads[0].wait()
    wide = image_ref[...].astype(F32)
    image_len = jnp.sqrt(jnp.sum(wide * wide, axis=-1, keepdims=True) + EPSILON)
    low = (wide / image_len).astype(BF16)
    img[rows(0, HALF), :] = low[:HALF]
    img[rows(256, HALF), :] = low[HALF:]

    pl.semaphore_wait(barrier, len(partners))

    ca, cb = {}, {}

    def sem_of(first, i, j):
        return r_first.at[first * 3 + i - 1] if j == 0 else r_second.at[first * 3 + j - 1]

    def ship_a(tx, ty, sx, where):
        ca[(tx, ty)] = send(img.at[rows(sx * HALF, HALF), :], img.at[rows((ty * 4 + tx) * HALF, HALF), :],
                            0, sem_of(0, tx, ty), where)

    def ship_b(tx, ty, sy, where):
        cb[(tx, ty)] = send(img.at[rows(256 + sy * HALF, HALF), :],
                            img.at[rows(256 + (tx * 4 + ty) * HALF, HALF), :],
                            0, sem_of(1, ty, tx), where)

    def pair(first, j):
        start = first * 256 + j * 64
        if j > 0:
            wait_all(img.at[rows(start, 64), :], r_second.at[first * 3 + j - 1])
        send(img.at[rows(start, 64), :], img.at[rows(512 + start, 64), :], 2, r_pair, at(dk=1))

    order = (1, 3, 2)
    for i in order:
        ship_a(4 - i, 0, 0, at(dx=i))
        ship_b(0, 4 - i, 0, at(dy=i))
    for i in order:
        ship_a(0, 4 - i, 0, at(dy=i))
        ship_b(4 - i, 0, 0, at(dx=i))

    loads[1].wait()
    loads[2].wait()
    projected = jnp.dot(text_ref[...], head[...], preferred_element_type=F32)
    text_len = jnp.sqrt(jnp.sum(projected * projected, axis=-1, keepdims=True) + EPSILON)
    text_dir = projected / text_len
    tdir[...] = text_dir
    txt[rows(0, ROWS), :] = text_dir.astype(BF16)

    cz = {}

    def ship_zc(sign, step, half, c):
        before = min(step - 1, 2)
        src_slot = ((8 - before) % 8) if sign > 0 else before
        dst_slot = (8 - step) if sign > 0 else step
        n = 16 if step > 2 else (((0 if sign > 0 else 2) + step - 1) * 2 + half) * 2 + c
        cz[(sign, step, half, c)] = send(
            txt.at[rows(TEXT_ROW[src_slot] + half * HALF, HALF), pl.ds(*CHUNKS[c])],
            txt.at[rows(TEXT_ROW[dst_slot] + half * HALF, HALF), pl.ds(*CHUNKS[c])],
            1, r_z.at[n], at(dz=sign * (step - before)))

    for half in range(2):
        for c in range(2):
            ship_zc(1, 1, half, c)
            ship_zc(-1, 1, half, c)

    def forward_image(i):
        ca[(i, 0)].wait_recv()
        for j in order:
            ship_a(i, 4 - j, i, at(dy=j))
        cb[(0, i)].wait_recv()
        for j in order:
            ship_b(4 - j, i, i, at(dx=j))

    column = lax.broadcasted_iota(jnp.int32, (1, COLS), 1)
    source = column
    for n in range(1, NZ):
        source = source + jnp.where(column >= n * SLICE, COLS - SLICE, 0)
    entry = lax.broadcasted_iota(jnp.int32, (D, COLS), 0)

    def select(q):
        chosen = jnp.where(entry == source + q * SLICE, 1.0, 0.0).astype(BF16)
        fsel_ref[q] = jnp.dot(text_ref[...], chosen, preferred_element_type=F32).astype(BF16)

    forward_image(3)
    forward_image(1)
    for step in (1, 2):
        for half in range(2):
            for c in range(2):
                for sign in (1, -1):
                    cz[(sign, step, half, c)].wait_recv()
                    if step == 2 and half == (0 if sign > 0 else 1):
                        ship_zc(sign, 4, half, c)
                    ship_zc(sign, step + 1, half, c)
        if step == 1:
            forward_image(2)
            pair(0, 0)
            pair(1, 0)
    pl.loop(4, 8)(select)
    for j in (1, 3, 2):
        pair(0, j)
        pair(1, j)
    factor = jnp.exp(jnp.full((1, 1), scale_ref[0], F32))
    offset = bias_ref[0]

    def weigh(i, core):
        part = rows(i * 128, 128)
        logits = factor * lax.dot_general(
            txt[part, :], img[rows(core * 512, 512), :], (((1,), (1,)), ((), ())),
            preferred_element_type=F32) + offset
        prob = jax.nn.sigmoid(logits)
        if i == 0 and core == 0:
            row = lax.broadcasted_iota(jnp.int32, (128, 512), 0)
            col = lax.broadcasted_iota(jnp.int32, (128, 512), 1)
            want = jnp.where(row < HALF, row, row + 240)
            prob = prob - jnp.where((row < ROWS) & (col == want), 1.0, 0.0).astype(F32)
        wt[part, pl.ds(core * 512, 512)] = (factor * prob).astype(BF16)

    def tile(i):
        part = rows(i * 128, 128)
        tp[part, :] = jnp.dot(wt[part, :], img[...], preferred_element_type=F32).astype(BF16)

    cr = {}

    def rz_slot(sign, dist, half):
        return ((0 if sign > 0 else 4) + dist - 1) * 2 + half

    def ship_rs(sign, dist, half, c):
        slot = dist if sign > 0 else (8 - dist)
        n = rz_slot(sign, dist, half)
        m = ((0 if sign > 0 else 2) + half) * 2 + c + 4 + 8 * (3 - dist)
        if dist == 4:
            m = (0 if sign > 0 else 2) + c
        cols = pl.ds(*CHUNKS[c])
        cr[(sign, dist, half, c)] = send(
            tp.at[rows(TEXT_ROW[slot] + half * HALF, HALF), cols], rz.at[n, :, cols],
            1, r_rs1 if dist < 3 else r_rs.at[m], at(dz=sign * (2 if dist in (2, 4) else 1)))

    def take_rs(sign, dists, half, c):
        slot = 2 if sign > 0 else 6
        part = rows(TEXT_ROW[slot] + half * HALF, HALF)
        cols = pl.ds(*CHUNKS[c])
        total = tp[part, cols].astype(F32)
        for dist in dists:
            cr[(sign, dist, half, c)].wait_recv()
            total = total + rz[rz_slot(sign, dist, half), :, cols].astype(F32)
        tp[part, cols] = total.astype(BF16)
        ship_rs(sign, 2, half, c)

    def image_tile(i):
        part = rows(i * 256, 256)
        ip[part, :] = lax.dot_general(
            wt[:, part], txt[...], (((0,), (0,)), ((), ())), preferred_element_type=F32).astype(BF16)

    ci = {}

    def ship_ir(name, dist, src, dst, n, where):
        ci[(name, dist)] = send(src, dst, 4, r_ir.at[n], where)

    def give_image(first):
        image_tile(2 + first)
        return send(ip.at[rows(512 + first * 256, 256), :], ipd.at[rows(first * 256, 256), :],
                    3, r_ex.at[first], at(dk=1))

    def join_image(first, copy):
        copy.wait_recv()

        def add(j):
            part = rows(pl.multiple_of(first * 256 + j * ROWS, ROWS), ROWS)
            ip[part, :] = (ip[part, :].astype(F32) + ipd[part, :].astype(F32)).astype(BF16)

        pl.loop(0, 8)(add)

    weigh(0, 0)
    wait_all(txt.at[rows(0, 96), :], r_z.at[16])
    weigh(1, 0)
    wait_all(img.at[rows(512, 512), :], r_pair)
    weigh(1, 1)
    tile(1)
    for c in range(2):
        ship_rs(1, 4, 0, c)
        ship_rs(-1, 4, 1, c)
        for half in range(2):
            ship_rs(1, 3, half, c)
            ship_rs(-1, 3, half, c)
    weigh(0, 1)
    tile(0)
    for c in range(2):
        for half in range(2):
            ship_rs(1, 1, half, c)
            ship_rs(-1, 1, half, c)
    ex = [give_image(0), give_image(1)]
    image_tile(0)
    image_tile(1)
    for c in range(2):
        take_rs(1, (4, 3), 0, c)
        take_rs(-1, (4, 3), 1, c)
        take_rs(1, (3,), 1, c)
        take_rs(-1, (3,), 0, c)
    join_image(0, ex[0])
    for i in order:
        ship_ir("ay", i, ip.at[rows(i * 64, 64), :], iay.at[i - 1], 0, at(dy=i))
    join_image(1, ex[1])
    for i in order:
        for j in range(4):
            ship_ir("by", i, ip.at[rows(256 + j * 64 + i * HALF, HALF), :],
                    iby.at[i - 1, rows(j * HALF, HALF), :], 1, at(dy=i))
    pl.loop(0, 4)(select)
    fall[0] = fsel_ref[k * 4 + x]
    for dk in range(2):
        for dx in range(4):
            if dk == 0 and dx == 0:
                continue
            slot = ((4 - dx) % 4) + 4 * dk
            send(fsel_ref.at[((k + dk) % 2) * 4 + (x + dx) % 4], fall.at[slot], 6, r_f, at(dx=dx, dk=dk))

    def fold(base, step, recv, sem):
        wait_all(recv, sem)
        for j in range(4):
            part = rows(base + j * step, HALF)
            total = ip[part, :].astype(F32)
            for i in range(3):
                total = total + recv[i, rows(j * HALF, HALF), :].astype(F32)
            ip[part, :] = total.astype(BF16)

    wait_all(rz.at[pl.ds(0, 8)], r_rs1)
    halves = []
    for half in range(2):
        total = tp[rows(half * HALF, HALF), :].astype(F32)
        for dist in (1, 2):
            for sign in (1, -1):
                total = total + rz[rz_slot(sign, dist, half)].astype(F32)
        halves.append(total)
    text_sum = jnp.concatenate(halves, axis=0)
    text_dir = tdir[...]
    proj_grad = (
        (text_sum - text_dir * jnp.sum(text_dir * text_sum, axis=-1, keepdims=True)) / text_len
    ).astype(BF16)
    pall[0] = proj_grad

    cp = {}
    for dx in order:
        slot = 4 - dx
        cp[slot] = send(pall.at[0], pall.at[slot], 5, r_p.at[slot - 1], at(dx=dx))
    send(pall.at[0], pall.at[4], 5, r_pk, at(dk=1))

    gt_ref[...] = lax.dot_general(
        proj_grad, head[...], (((1,), (1,)), ((), ())), preferred_element_type=F32).astype(BF16)

    for slot in (1, 3, 2):
        cp[slot].wait_recv()
        send(pall.at[slot], pall.at[4 + slot], 5, r_pk, at(dk=1))
    wait_all(pall.at[pl.ds(4, 4)], r_pk)
    wait_all(fall.at[pl.ds(1, 7)], r_f)

    hp[...] = lax.dot_general(
        fall[...].reshape(256, COLS), pall[...].reshape(256, D), (((0,), (0,)), ((), ())),
        preferred_element_type=F32)
    for s in range(NZ):
        part = hp[rows(s * SLICE, SLICE), :]
        hm[s] = part[:HALF].astype(BF16)
        hl[s] = part[HALF:].astype(BF16)
    far = (4, 3, 5, 2, 6, 1, 7)
    for c in range(2):
        cols = pl.ds(*PIECES[c])
        for dz in far:
            dest = (z + dz) % NZ
            send(hm.at[dest, :, cols], rm.at[dz, :, cols], 7, r_hm.at[c], at(dz=dz))
            if c == 0:
                send(hl.at[dest], rl.at[dz], 8, r_hl, at(dz=dz))

    fold(0, HALF, iay, r_ir.at[0])
    fold(256, 64, iby, r_ir.at[1])
    for i in order:
        ship_ir("ax", i, ip.at[rows(i * HALF, HALF), :], iax.at[i - 1], 2, at(dx=i))
        ship_ir("bx", i, ip.at[rows(256 + i * 64, HALF), :], ibx.at[i - 1], 3, at(dx=i))
    y_lo = y % 2

    def piece(p, slot):
        if p == 2:
            return sl, ql.at[slot]
        return sm.at[:, pl.ds(*PIECES[p])], qm.at[slot, :, pl.ds(*PIECES[p])]

    def final(p, target_y, target_k, slot):
        src, dst = piece(p, slot)
        return pltpu.make_async_remote_copy(
            src_ref=src, dst_ref=dst, send_sem=s_q.at[p * 4 + target_y // 2 * 2 + target_k],
            recv_sem=r_q.at[p * 4 + slot], device_id=device(x, target_y, z, target_k), device_id_type=MESH)

    def scatter(pieces):
        for h in range(2):
            for tk in range(2):
                ty = k + 2 * h
                own = (ty == y) & (tk == k)

                @pl.when(jnp.logical_not(own))
                def _():
                    for p in pieces:
                        final(p, ty, tk, y).start()

                @pl.when(own)
                def _():
                    for p in pieces:
                        src, dst = piece(p, y)
                        dst[...] = src[...]

    def collect(pieces):
        for sy in range(4):
            @pl.when(jnp.logical_not((sy == y) & (k == y_lo)))
            def _():
                for p in pieces:
                    final(p, y, k, sy).wait_recv()

    def sum_z(own, recv):
        total = own.astype(F32)
        for dz in far:
            total = total + recv(dz).astype(F32)
        return total.astype(BF16)

    def sum_y(part):
        total = part(0).astype(F32)
        for sy in range(1, 4):
            total = total + part(sy).astype(F32)
        return total

    def finish_image():
        wait_all(iax, r_ir.at[2])
        wait_all(ibx, r_ir.at[3])
        total_a = ip[rows(0, HALF), :].astype(F32)
        total_b = ip[rows(256, HALF), :].astype(F32)
        for i in range(3):
            total_a = total_a + iax[i].astype(F32)
            total_b = total_b + ibx[i].astype(F32)
        image_sum = jnp.concatenate([total_a, total_b], axis=0)
        wide = image_ref[...].astype(F32)
        image_len = jnp.sqrt(jnp.sum(wide * wide, axis=-1, keepdims=True) + EPSILON)
        image_dir = wide / image_len
        gi_ref[...] = (
            (image_sum - image_dir * jnp.sum(image_dir * image_sum, axis=-1, keepdims=True)) / image_len
        ).astype(BF16)

    for c in range(2):
        cols = pl.ds(*PIECES[c])
        wait_all(rm.at[pl.ds(1, 7), :, cols], r_hm.at[c])
        sm[:, cols] = sum_z(hm[z, :, cols], lambda dz: rm[dz, :, cols])
        if c == 0:
            wait_all(rl.at[pl.ds(1, 7)], r_hl)
            sl[...] = sum_z(hl[z], lambda dz: rl[dz])
        scatter((0, 2) if c == 0 else (1,))
        if c == 0:
            finish_image()
    for c in range(2):
        cols = pl.ds(*PIECES[c])
        collect((0, 2) if c == 0 else (1,))
        gh_ref[pl.ds(0, HALF), cols] = sum_y(lambda sy: qm[sy, :, cols])
        if c == 0:
            gh_ref[pl.ds(HALF, 2), :] = sum_y(lambda sy: ql[sy])

    for n, ref in enumerate((
        img.at[rows(0, 480), :],
        img.at[rows(0, 448), :],
        img.at[rows(0, 512), :],
        img.at[rows(0, 512), :],
        img.at[rows(0, 480), :],
        pall.at[pl.ds(0, 7)],
        fall.at[pl.ds(0, 7)],
        rm.at[pl.ds(0, 7)],
        rl.at[pl.ds(0, 7)],
    )):
        wait_all(ref, s_all.at[n])
    for h in range(2):
        for tk in range(2):
            ty = k + 2 * h

            @pl.when(jnp.logical_not((ty == y) & (tk == k)))
            def _():
                for p in range(3):
                    final(p, ty, tk, y).wait_send()


def deliver(gi_ref, gt_ref, gh_ref, gi_out, gt_out, gh_out, sem):
    copies = [
        pltpu.make_async_copy(src, dst, sem.at[n])
        for n, (src, dst) in enumerate(((gi_ref, gi_out), (gt_ref, gt_out), (gh_ref, gh_out)))
    ]
    for copy in copies:
        copy.start()
    for copy in copies:
        copy.wait()


def local(image_embed, text_feature, text_head, log_scale, bias):
    hbm = pl.BlockSpec(memory_space=pltpu.HBM)
    vmem = pl.BlockSpec(memory_space=pltpu.VMEM)
    dma = pltpu.SemaphoreType.DMA
    V = pltpu.VMEM
    shapes = (
        jax.ShapeDtypeStruct((ROWS, D), BF16),
        jax.ShapeDtypeStruct((ROWS, D), BF16),
        jax.ShapeDtypeStruct((SLICE, D), F32),
    )
    results = pl.pallas_call(
        kernel,
        out_shape=tuple(pltpu.VMEM(a.shape, a.dtype) for a in shapes),
        in_specs=[pl.BlockSpec(memory_space=pltpu.SMEM)] * 2 + [hbm] * 3,
        out_specs=(vmem, vmem, vmem),
        scratch_shapes=[
            V((ROWS, D), BF16),
            V((ROWS, D), BF16),
            V((8, ROWS, COLS), BF16),
            V((D, D), BF16),
            V((IMAGES, D), BF16),
            V((TEXTS, D), BF16),
            V((TEXTS, IMAGES), BF16),
            V((TEXTS, D), BF16),
            V((IMAGES, D), BF16),
            V((16, HALF, D), BF16),
            V((3, 64, D), BF16),
            V((3, HALF, D), BF16),
            V((3, 64, D), BF16),
            V((3, HALF, D), BF16),
            V((512, D), BF16),
            V((ROWS, D), F32),
            V((8, ROWS, D), BF16),
            V((8, ROWS, COLS), BF16),
            V((COLS, D), F32),
            V((NZ, HALF, D), BF16),
            V((NZ, 2, D), BF16),
            V((NZ, HALF, D), BF16),
            V((NZ, 2, D), BF16),
            V((HALF, D), BF16),
            V((2, D), BF16),
            V((4, HALF, D), BF16),
            V((4, 2, D), BF16),
            dma((3,)),
            dma((6,)), dma((6,)), dma, dma((17,)), dma, dma((12,)), dma, dma((2,)), dma((4,)),
            dma((3,)), dma, dma((2,)), dma, dma((12,)), dma((12,)), dma((9,)),
        ],
        compiler_params=pltpu.CompilerParams(
            collective_id=0, has_side_effects=True, vmem_limit_bytes=66500000),
        name="contrastive",
    )(log_scale, bias, image_embed, text_feature, text_head)
    return pl.pallas_call(
        deliver,
        out_shape=shapes,
        in_specs=[vmem] * 3,
        out_specs=(hbm, hbm, hbm),
        scratch_shapes=[dma((3,))],
        compiler_params=pltpu.CompilerParams(vmem_limit_bytes=2**20),
        name="deliver",
    )(*results)


def solution(mesh):
    both = P(("grp", "blk"), None)
    return jax.shard_map(
        local,
        mesh=mesh,
        in_specs=(both, both, P(), P(), P()),
        out_specs=(both, both, P("blk", None)),
        check_vma=False,
    )
```
